32 devices in a mesh: gx: 4 (over y, x), gy: 2 (over core), gz: 4 (over z).
Axes of the slice: x: 2, y: 2, z: 4, core: 2. Of those that a mesh axis runs over, the one named last changes fastest.
Arguments:
- gradient: float32 [4, 2, 4, 16, 512], P('gx', 'gy', 'gz'), may hold values from -60 to 60
- local_schur: bfloat16 [4, 2, 4, 2048, 2048], P('gx', 'gy', 'gz'), may hold values from -1 to 4
- inverse_rows: bfloat16 [4, 2, 4, 512, 2048], P('gx', 'gy', 'gz'), may hold values from -0.1 to 0.6
- face_maps: int32 [4, 2, 4, 6, 256], P('gx', 'gy', 'gz'), may hold values from 0 to 511, as said below
Outputs:
- adjoint: float32 [4, 2, 4, 16, 512], P('gx', 'gy', 'gz')
- residual_ratio: float32 [16], replicated
The draws below stay inside these ranges and needn't reach their ends.
Inputs may be any that keep to these rules, and one draw needn't show every extreme that they name: `face_maps`: for each subdomain and face, 256 distinct owned rows of the neighbour across that face.
All inputs are finite; a program needn't handle non-finite values.
Results may differ from the reference program's by a relative error of at most 0.0038.
Values may be sent and summed in bfloat16 or wider, within the bound.
A program may use at most 64 MiB of HBM per device.

```python
import math
import jax
import jax.numpy as jnp
from jax import lax

M = 2048
OWN = 512
RHS = 16
ITERS = 3
FACE = 256
SX = 4
SY = 2
SZ = 4


def device_ramp(highest):
    devices_n = SX * SY * SZ
    flat_ids = jnp.arange(devices_n, dtype=jnp.float32).reshape(SX, SY, SZ, 1, 1)
    return 1.0 + (highest - 1.0) * flat_ids / max(devices_n - 1, 1)


def draw_gradient(key, part):
    subkeys = jax.random.split(jax.random.fold_in(key, 11), 3)
    shape = (SX, SY, SZ, RHS, OWN)
    row_scale = jnp.exp(jax.random.uniform(subkeys[1], (SX, SY, SZ, 1, OWN), jnp.float32, math.log(0.3), math.log(3.0)))
    rhs_scale = jnp.exp(jax.random.uniform(subkeys[2], (1, 1, 1, RHS, 1), jnp.float32, math.log(0.5), math.log(1.5)))
    base_vals = jnp.clip(jax.random.normal(subkeys[0], shape, jnp.float32), -4.0, 4.0)
    ramp_vals = device_ramp(3.0)
    return base_vals * row_scale * rhs_scale * ramp_vals


def draw_local_schur(key, part):
    subkeys = jax.random.split(jax.random.fold_in(key, 23), 2)
    shape = (SX, SY, SZ, M, M)
    sigma = 0.6 / math.sqrt(M)
    noise = jnp.clip(jax.random.normal(subkeys[0], shape, jnp.float32), -4.0, 4.0) * sigma
    diagonal = jax.random.uniform(subkeys[1], (SX, SY, SZ, 1, M), jnp.float32, 1.0, 3.0)
    identity = (jnp.arange(M)[:, None] == jnp.arange(M)[None, :]).astype(jnp.float32)
    return (noise + diagonal * identity).astype(jnp.bfloat16)


def draw_inverse_rows(key, part):
    subkeys = jax.random.split(jax.random.fold_in(key, 37), 2)
    shape = (SX, SY, SZ, OWN, M)
    sigma = 0.1 / math.sqrt(M)
    noise = jnp.clip(jax.random.normal(subkeys[0], shape, jnp.float32), -4.0, 4.0) * sigma
    diagonal = jnp.exp(jax.random.uniform(subkeys[1], (SX, SY, SZ, OWN, 1), jnp.float32, math.log(0.1), math.log(0.5)))
    identity = (jnp.arange(OWN)[:, None] == jnp.arange(M)[None, :]).astype(jnp.float32)
    return (noise + diagonal * identity).astype(jnp.bfloat16)


def draw_face_maps(key, part):
    scores = jax.random.randint(jax.random.fold_in(key, 53), (SX, SY, SZ, 6, OWN), 0, 1 << 20, jnp.int32)
    scores = scores * OWN + jnp.arange(OWN, dtype=jnp.int32)
    return jnp.argsort(scores, axis=-1)[..., :FACE].astype(jnp.int32)


def setup_inputs(seed: int = 0) -> dict:
    streams_of = jax.random.split(jax.random.key(seed), 5)
    gradient = draw_gradient(jax.random.fold_in(streams_of[4], 71), 0)
    local_schur = draw_local_schur(jax.random.fold_in(streams_of[4], 71), 0)
    inverse_rows = draw_inverse_rows(jax.random.fold_in(streams_of[4], 71), 0)
    face_maps = draw_face_maps(jax.random.fold_in(streams_of[4], 71), 0)
    return {"gradient": gradient, "local_schur": local_schur, "inverse_rows": inverse_rows, "face_maps": face_maps}


EPSILON = 1e-06

def across(values, facing):
    dimension = facing // 2
    widths = [(0, 0)] * values.ndim
    extent = values.shape[dimension]
    if facing % 2 == 0:
        widths[dimension] = (1, 0)
        return lax.slice_in_dim(jnp.pad(values, widths), 0, extent, axis=dimension)
    widths[dimension] = (0, 1)
    return lax.slice_in_dim(jnp.pad(values, widths), 1, extent + 1, axis=dimension)

def flatten_grid(values):
    return values.reshape((-1,) + values.shape[3:])

def take_rows(face_block, row_ids):
    return jnp.take(face_block, row_ids, axis=1)

def add_rows(face_block, row_ids, addition):
    return face_block.at[:, row_ids].add(addition)

def multiply_pair(operands):
    return jnp.dot(operands[0], operands[1], preferred_element_type=jnp.float32)

def assemble(products, face_maps):
    owned = products.shape[-1] - 6 * FACE
    result = flatten_grid(products[..., :owned])
    for facing in range(6):
        offset = owned + (facing ^ 1) * FACE
        face_block = across(products[..., offset:offset + FACE], facing)
        row_ids = across(face_maps[..., facing ^ 1, :], facing)
        result = jax.vmap(add_rows)(result, flatten_grid(row_ids), flatten_grid(face_block))
    return result.reshape(products.shape[:-1] + (owned,))

def operator(values, face_maps, local_schur):
    rounded = values.astype(jnp.bfloat16)
    ghosts = [jax.vmap(take_rows)(flatten_grid(across(rounded, facing)), flatten_grid(face_maps[..., facing, :])) for facing in range(6)]
    intersected = jnp.concatenate([flatten_grid(rounded)] + ghosts, axis=2)
    products = lax.map(multiply_pair, (intersected, flatten_grid(local_schur)))
    return assemble(products.reshape(values.shape[:3] + products.shape[1:]), face_maps)

def precondition(values, face_maps, inverse_rows):
    rounded = flatten_grid(values.astype(jnp.bfloat16))
    products = lax.map(multiply_pair, (rounded, flatten_grid(inverse_rows)))
    return assemble(products.reshape(values.shape[:3] + products.shape[1:]), face_maps)

def inner_sum(left_side, right_side):
    return lax.optimization_barrier(jnp.sum(left_side * right_side, axis=(0, 1, 2, 4)))

def rotate_solve(columns, beta_norm):
    num_cols = len(columns)
    rhs_vec = [beta_norm] + [jnp.zeros_like(beta_norm) for unused in range(num_cols)]
    cosines = []
    sines = []
    triangle = []
    for section in range(num_cols):
        column = [columns[section][row_at] for row_at in range(section + 2)]
        for earlier in range(section):
            rotated_a = cosines[earlier] * column[earlier] + sines[earlier] * column[earlier + 1]
            rotated_b = -sines[earlier] * column[earlier] + cosines[earlier] * column[earlier + 1]
            column[earlier] = rotated_a
            column[earlier + 1] = rotated_b
        radius = jnp.sqrt(column[section] * column[section] + column[section + 1] * column[section + 1])
        cosine = column[section] / radius
        sine_val = column[section + 1] / radius
        column[section] = radius
        cosines.append(cosine)
        sines.append(sine_val)
        rhs_vec[section + 1] = -sine_val * rhs_vec[section]
        rhs_vec[section] = cosine * rhs_vec[section]
        triangle.append(column[:section + 1])
    coeffs = [None] * num_cols
    for section in reversed(range(num_cols)):
        running = rhs_vec[section]
        for onward in range(section + 1, num_cols):
            running = running - triangle[onward][section] * coeffs[onward]
        coeffs[section] = running / triangle[section][section]
    return (coeffs, jnp.abs(rhs_vec[num_cols]))

def reference(gradient, local_schur, inverse_rows, face_maps):
    beta_norm = jnp.sqrt(inner_sum(gradient, gradient) + EPSILON)
    krylov = [gradient / beta_norm[:, None]]
    directions = []
    columns = []
    for section in range(ITERS):
        prepared = precondition(krylov[section], face_maps, inverse_rows)
        directions.append(prepared)
        applied = operator(prepared, face_maps, local_schur)
        coeffs = [inner_sum(vector, applied) for vector in krylov]
        residue = applied
        for position in range(section + 1):
            residue = residue - coeffs[position][:, None] * krylov[position]
        height = jnp.sqrt(inner_sum(residue, residue) + EPSILON)
        columns.append(coeffs + [height])
        if section + 1 < ITERS:
            krylov.append(residue / height[:, None])
    weights, remainder = rotate_solve(columns, beta_norm)
    adjoint = weights[0][:, None] * directions[0]
    for position in range(1, ITERS):
        adjoint = adjoint + weights[position][:, None] * directions[position]
    return (adjoint, remainder / beta_norm)
```

```python
import functools

import jax
import jax.numpy as jnp
from jax import lax
from jax.experimental import pallas as pl
from jax.experimental.pallas import tpu as pltpu
from jax.sharding import PartitionSpec as P

ITERS = 3
EPSILON = 1e-06
MESH = pl.DeviceIdType.MESH
BF16 = jnp.bfloat16
F32 = jnp.float32
DIRECT_MAX = 32


def split(x):
    high = x.astype(BF16)
    low = (x - high.astype(F32)).astype(BF16)
    return jnp.concatenate([high, low], axis=0)


def merge(x):
    rows = x.shape[0] // 2
    return x[:rows] + x[rows:]


def mm(a, b):
    return jnp.dot(a, b, preferred_element_type=F32)


def rotate_column(column, section, cosines, sines, rhs_vec, triangle):
    column = list(column)
    for earlier in range(section):
        rotated_a = cosines[earlier] * column[earlier] + sines[earlier] * column[earlier + 1]
        rotated_b = -sines[earlier] * column[earlier] + cosines[earlier] * column[earlier + 1]
        column[earlier] = rotated_a
        column[earlier + 1] = rotated_b
    radius = jnp.sqrt(
        column[section] * column[section] + column[section + 1] * column[section + 1]
    )
    cosine = column[section] / radius
    sine_val = column[section + 1] / radius
    column[section] = radius
    cosines.append(cosine)
    sines.append(sine_val)
    rhs_vec[section + 1] = -sine_val * rhs_vec[section]
    rhs_vec[section] = cosine * rhs_vec[section]
    triangle.append(column[: section + 1])


def back_substitute(rhs_vec, triangle):
    num_cols = len(triangle)
    coeffs = [None] * num_cols
    for section in reversed(range(num_cols)):
        running = rhs_vec[section]
        for onward in range(section + 1, num_cols):
            running = running - triangle[onward][section] * coeffs[onward]
        coeffs[section] = running / triangle[section][section]
    return coeffs


class Axis:
    def __init__(self, axis, spot, size, own, face, at):
        self.axis = axis
        self.single = size == 2
        low, high = spot > 0, spot < size - 1
        if self.single:
            which = 2 * axis + jnp.where(low, 0, 1)
            self.faces = [(2 * axis, 2 * axis, which, None, jnp.where(low, -1, 1))]
            self.width = face
            self.start = pl.multiple_of(own + which * face, face)
        else:
            self.faces = [
                (2 * axis, 2 * axis + 1, 2 * axis, low, -1),
                (2 * axis + 1, 2 * axis, 2 * axis + 1, high, 1),
            ]
            self.width = 2 * face
            self.start = own + 2 * axis * face
        self.columns = pl.ds(self.start, self.width)
        self.packed = pl.ds(at, self.width)


def kernel(
    sizes, g_ref, maps_ref, k_hbm, b_hbm, out_ref,
    k_ref, b_ref, near_maps, gather_ref, scatter_ref, send_buf, recv_buf, acc_ref,
    base_ref, t_ref, v_ref, z_ref, w_ref, last_ref, total_ref, plane_buf, line_buf, all_buf,
    weight_sem, map_send, map_recv, send_sem, recv_sem,
    plane_send, plane_recv, line_send, line_recv, all_send, all_recv,
):
    nx, ny, nz = sizes
    count = nx * ny * nz
    direct = count <= DIRECT_MAX
    rhs, own = g_ref.shape
    face = maps_ref.shape[-1]
    whole = k_ref.shape[0]
    ix, iy, iz = lax.axis_index("gx"), lax.axis_index("gy"), lax.axis_index("gz")
    here = (ix, iy, iz)

    groups = []
    at = 0
    for axis in range(3):
        if sizes[axis] > 1:
            groups.append(Axis(axis, here[axis], sizes[axis], own, face, at))
            at += groups[-1].width
    sending = [group for axis in (0, 2, 1) for group in groups if group.axis == axis]
    arriving = [group for axis in (1, 2, 0) for group in groups if group.axis == axis]
    final = arriving[-1]
    own_columns = pl.ds(0, own)

    def across(axis, step):
        place = list(here)
        place[axis] = place[axis] + step
        return tuple(place)

    def guarded(exists, body):
        if exists is None:
            body()
        else:
            pl.when(exists)(body)

    plane = [
        (lax.rem(ix + dx, nx), lax.rem(iy + dy, ny))
        for dx in range(nx) for dy in range(ny) if dx or dy
    ]
    line = [lax.rem(iz + dz, nz) for dz in range(1, nz)]
    others = [
        (lax.rem(ix + dx, nx), lax.rem(iy + dy, ny), lax.rem(iz + dz, nz))
        for dx in range(nx) for dy in range(ny) for dz in range(nz) if dx or dy or dz
    ]

    load_b = pltpu.make_async_copy(b_hbm, b_ref, weight_sem.at[0])
    load_own = pltpu.make_async_copy(
        k_hbm.at[pl.ds(0, own)], k_ref.at[pl.ds(0, own)], weight_sem.at[1]
    )
    ghosts = pl.ds(own, whole - own)
    load_ghosts = pltpu.make_async_copy(k_hbm.at[ghosts], k_ref.at[ghosts], weight_sem.at[2])
    load_b.start()

    barrier = pltpu.get_barrier_semaphore()
    greeted = [(px, py, iz) for px, py in plane] + [(ix, iy, pz) for pz in line]
    for peer in greeted:
        pl.semaphore_signal(barrier, inc=1, device_id=peer, device_id_type=MESH)

    t_ref[...] = g_ref[...]
    v_ref[...] = jnp.zeros_like(v_ref)
    z_ref[...] = jnp.zeros_like(z_ref)
    w_ref[...] = jnp.zeros_like(w_ref)
    last_ref[...] = jnp.zeros_like(last_ref)
    total_ref[...] = jnp.zeros_like(total_ref)
    for group in groups:
        for slot, _, _, exists, _ in group.faces:
            if exists is not None:
                @pl.when(jnp.logical_not(exists))
                def _():
                    near_maps[slot] = jnp.full(near_maps.shape[1:], -1, jnp.int32)
                    for e in range(3 * ITERS):
                        recv_buf[e, slot] = jnp.zeros(recv_buf.shape[2:], BF16)

    def map_copy(group, entry):
        slot, target, which, _, step = entry
        return pltpu.make_async_remote_copy(
            src_ref=maps_ref.at[which], dst_ref=near_maps.at[target],
            send_sem=map_send.at[slot], recv_sem=map_recv.at[target],
            device_id=across(group.axis, step), device_id_type=MESH,
        )

    def map_wait(group, entry):
        slot, _, which, _, step = entry
        return pltpu.make_async_remote_copy(
            src_ref=maps_ref.at[which], dst_ref=near_maps.at[slot],
            send_sem=map_send.at[slot], recv_sem=map_recv.at[slot],
            device_id=across(group.axis, step), device_id_type=MESH,
        )

    def face_copy(e, group, entry, arrival=False):
        slot, target, _, _, step = entry
        into = slot if arrival else target
        return pltpu.make_async_remote_copy(
            src_ref=send_buf.at[e, slot], dst_ref=recv_buf.at[e, into],
            send_sem=send_sem.at[e, slot], recv_sem=recv_sem.at[e, into],
            device_id=across(group.axis, step), device_id_type=MESH,
        )

    def plane_copy(r, peer, slot):
        mine = ix * ny + iy
        return pltpu.make_async_remote_copy(
            src_ref=plane_buf.at[r, mine], dst_ref=plane_buf.at[r, slot],
            send_sem=plane_send.at[r, peer[0] * ny + peer[1]], recv_sem=plane_recv.at[r, slot],
            device_id=(peer[0], peer[1], iz), device_id_type=MESH,
        )

    def line_copy(r, peer, slot):
        return pltpu.make_async_remote_copy(
            src_ref=line_buf.at[r, iz], dst_ref=line_buf.at[r, slot],
            send_sem=line_send.at[r, peer], recv_sem=line_recv.at[r, slot],
            device_id=(ix, iy, peer), device_id_type=MESH,
        )

    def rank(peer):
        return (peer[0] * ny + peer[1]) * nz + peer[2]

    def all_copy(peer, slot):
        return pltpu.make_async_remote_copy(
            src_ref=all_buf.at[rank(here)], dst_ref=all_buf.at[slot],
            send_sem=all_send.at[rank(peer)], recv_sem=all_recv.at[slot],
            device_id=peer, device_id_type=MESH,
        )

    lanes = lax.broadcasted_iota(jnp.int32, (rhs, 128), 1)
    rows = lax.broadcasted_iota(jnp.int32, (rhs, 128), 0)
    spread = 128 // rhs
    places = lax.rem(lanes, spread)
    mine = lax.div(lanes, spread) == rows

    def packed_sums():
        t = t_ref[...]
        last = last_ref[...]
        packed = jnp.where(places == ITERS, jnp.sum(t * t, axis=1, keepdims=True), 0.0)
        for k in range(ITERS):
            v = v_ref[k]
            packed = jnp.where(places == k, jnp.sum(v * t, axis=1, keepdims=True), packed)
            packed = jnp.where(
                places == ITERS + 1 + k, jnp.sum(v * last, axis=1, keepdims=True), packed
            )
        return jnp.sum(jnp.where(mine, packed, 0.0), axis=0, keepdims=True)

    def start_sums(r):
        plane_buf[r, ix * ny + iy] = packed_sums()
        for peer in plane:
            plane_copy(r, peer, ix * ny + iy).start()

    def pass_sums(r):
        for peer in plane:
            plane_copy(r, peer, peer[0] * ny + peer[1]).wait_recv()
        partial = plane_buf[r, 0]
        for at in range(1, nx * ny):
            partial = partial + plane_buf[r, at]
        line_buf[r, iz] = partial
        for peer in line:
            line_copy(r, peer, iz).start()

    def finish_sums(r):
        for peer in line:
            line_copy(r, peer, peer).wait_recv()
        total = line_buf[r, 0]
        for at in range(1, nz):
            total = total + line_buf[r, at]
        total_ref[r] = jnp.where(mine, total, 0.0)

    def pick(r, lane):
        return jnp.sum(jnp.where(places == lane, total_ref[r], 0.0), axis=1, keepdims=True)

    def heights(r, count):
        coeffs = [pick(r, k) for k in range(count)]
        running = pick(r, ITERS)
        for k in range(count):
            running = running - 2.0 * coeffs[k] * coeffs[k]
            for n in range(k + 1):
                element = coeffs[k] * pick(k + 1, ITERS + 1 + n) * coeffs[n]
                running = running + (element if n == k else 2.0 * element)
        return coeffs, jnp.sqrt(jnp.maximum(running, 0.0) + EPSILON)

    def arrived(e, group):
        for entry in group.faces:
            guarded(entry[3], lambda: face_copy(e, group, entry, True).wait_recv())
        blocks = [recv_buf[e, entry[0]] for entry in group.faces]
        return blocks[0] if len(blocks) == 1 else jnp.concatenate(blocks, axis=1)

    def scattered(e, base):
        for group in arriving:
            base = base + mm(arrived(e, group), scatter_ref[group.packed, :])
        return base

    def send(e, group, values):
        values = values.astype(BF16)
        for at, entry in enumerate(group.faces):
            send_buf[e, entry[0]] = values[:, at * face : (at + 1) * face]

        def start(entry, when=None):
            exists = entry[3]
            if when is not None:
                exists = when if exists is None else jnp.logical_and(exists, when)
            guarded(exists, lambda: face_copy(e, group, entry).start())

        if group is final and len(group.faces) == 2:
            odd = lax.rem(here[group.axis], 2) == 1
            start(group.faces[1], odd)
            start(group.faces[0])
            start(group.faces[1], jnp.logical_not(odd))
        else:
            for entry in group.faces:
                start(entry)

    def precondition(e, ready):
        pair = split(t_ref[...])
        first = True
        for group in sending:
            values = merge(mm(pair, b_ref[:, group.columns]))
            if first:
                ready()
                first = False
            send(e, group, values)
        base_ref[...] = merge(mm(pair, b_ref[:, own_columns]))

    def iteration(j, carry):
        first, second, third = 3 * j, 3 * j + 1, 3 * j + 2
        start_sums(j)

        @pl.when(j == 0)
        def _():
            for group in groups:
                for at, entry in enumerate(group.faces):
                    guarded(entry[3], lambda: map_wait(group, entry).wait_recv())
                    row = near_maps[entry[0]]
                    hot = lax.broadcasted_iota(jnp.int32, (own, face), 0) == row
                    hot = jnp.where(hot, 1.0, 0.0)
                    part = pl.ds(group.packed.start + at * face, face)
                    gather_ref[:, part] = hot.astype(BF16)
                    scatter_ref[part, :] = jnp.transpose(hot).astype(BF16)

        prepared = scattered(first, base_ref[...])
        rounded = prepared.astype(BF16)
        for group in sending:
            send(second, group, mm(rounded, gather_ref[:, group.packed]))
        pair = split(prepared)
        pass_sums(j)

        @pl.when(j == 0)
        def _():
            load_own.wait()

        targets = [group.columns for group in sending] + [own_columns]
        for columns in targets:
            acc_ref[:, columns] = merge(mm(pair, k_ref[own_columns, columns]))

        @pl.when(j == 0)
        def _():
            load_ghosts.wait()

        for group in arriving[:-1]:
            values = arrived(second, group)
            for columns in targets:
                acc_ref[:, columns] += mm(values, k_ref[group.columns, columns])
        values = arrived(second, final)

        def products(columns):
            return acc_ref[:, columns] + mm(values, k_ref[final.columns, columns])

        for group in sending:
            send(third, group, products(group.columns))
        base = products(own_columns)
        finish_sums(j)
        coeffs, height = heights(j, ITERS - 1)
        inverse = 1.0 / height
        newest = t_ref[...]
        for k in range(ITERS - 1):
            prepared = prepared - coeffs[k] * z_ref[k]
            newest = newest - coeffs[k] * v_ref[k]
        z_ref[j] = prepared * inverse
        newest = newest * inverse
        v_ref[j] = newest
        last_ref[...] = newest
        applied = scattered(third, base)
        for k in range(ITERS - 1):
            applied = applied - coeffs[k] * w_ref[k]
        applied = applied * inverse
        w_ref[j] = applied
        t_ref[...] = applied

        @pl.when(j < ITERS - 1)
        def _():
            precondition(3 * j + 3, lambda: None)

        return carry

    def ready():
        load_own.start()
        load_ghosts.start()
        pl.semaphore_wait(barrier, len(greeted))
        for group in groups:
            for entry in group.faces:
                guarded(entry[3], lambda: map_copy(group, entry).start())

    load_b.wait()
    precondition(0, ready)
    lax.fori_loop(0, ITERS, iteration, 0)
    if direct:
        all_buf[rank(here)] = packed_sums()
        for peer in others:
            all_copy(peer, rank(here)).start()
    else:
        start_sums(ITERS)
        pass_sums(ITERS)
    beta_norm = heights(0, 0)[1]
    rhs_vec = [beta_norm] + [jnp.zeros_like(beta_norm)] * ITERS
    cosines, sines, triangle = [], [], []
    for section in range(ITERS - 1):
        coeffs, height = heights(section + 1, section + 1)
        rotate_column(coeffs + [height], section, cosines, sines, rhs_vec, triangle)
    if direct:
        for peer in others:
            all_copy(peer, rank(peer)).wait_recv()
        total = jnp.sum(all_buf[...], axis=0)
        total_ref[ITERS] = jnp.where(mine, total, 0.0)
    else:
        finish_sums(ITERS)
    coeffs, height = heights(ITERS, ITERS)
    rotate_column(coeffs + [height], ITERS - 1, cosines, sines, rhs_vec, triangle)
    solved = back_substitute(rhs_vec, triangle)
    adjoint = solved[0] * z_ref[0]
    for k in range(1, ITERS):
        adjoint = adjoint + solved[k] * z_ref[k]
    out_ref[pl.ds(0, rhs), :] = adjoint
    ratio = jnp.abs(rhs_vec[ITERS]) / beta_norm
    ratio = jnp.sum(jnp.where(rows == lanes, ratio, 0.0), axis=0, keepdims=True)
    out_ref[pl.ds(rhs, 8), pl.ds(0, 128)] = jnp.broadcast_to(ratio, (8, 128))

    for group in groups:
        for entry in group.faces:
            def drain():
                map_copy(group, entry).wait_send()
                for e in range(3 * ITERS):
                    face_copy(e, group, entry).wait_send()
            guarded(entry[3], drain)
    for r in range(ITERS if direct else ITERS + 1):
        for peer in plane:
            plane_copy(r, peer, ix * ny + iy).wait_send()
        for peer in line:
            line_copy(r, peer, iz).wait_send()
    if direct:
        for peer in others:
            all_copy(peer, rank(here)).wait_send()


def local(sizes, gradient, local_schur, inverse_rows, face_maps):
    nx, ny, nz = sizes
    target = gradient[0, 0, 0]
    rhs, own = target.shape
    maps = jnp.swapaxes(face_maps[0, 0], 0, 1)
    face = maps.shape[-1]
    whole = local_schur.shape[-1]
    exchanges = 3 * ITERS
    sums = ITERS + 1
    count = nx * ny * nz
    direct = count if count <= DIRECT_MAX else 1
    vmem = pl.BlockSpec(memory_space=pltpu.VMEM)
    hbm = pl.BlockSpec(memory_space=pl.ANY)
    dma = pltpu.SemaphoreType.DMA
    packed = pl.pallas_call(
        functools.partial(kernel, sizes),
        out_shape=pltpu.VMEM((rhs + 8, own), F32),
        in_specs=[vmem, vmem, hbm, hbm],
        out_specs=vmem,
        scratch_shapes=[
            pltpu.VMEM((whole, whole), BF16),
            pltpu.VMEM((own, whole), BF16),
            pltpu.VMEM(maps.shape, jnp.int32),
            pltpu.VMEM((own, 6 * face), BF16),
            pltpu.VMEM((6 * face, own), BF16),
            pltpu.VMEM((exchanges, 6, rhs, face), BF16),
            pltpu.VMEM((exchanges, 6, rhs, face), BF16),
            pltpu.VMEM((rhs, whole), F32),
            pltpu.VMEM((rhs, own), F32),
            pltpu.VMEM((rhs, own), F32),
            pltpu.VMEM((ITERS, rhs, own), F32),
            pltpu.VMEM((ITERS, rhs, own), F32),
            pltpu.VMEM((ITERS, rhs, own), F32),
            pltpu.VMEM((rhs, own), F32),
            pltpu.VMEM((sums, rhs, 128), F32),
            pltpu.VMEM((sums, nx * ny, 1, 128), F32),
            pltpu.VMEM((sums, nz, 1, 128), F32),
            pltpu.VMEM((direct, 1, 128), F32),
            dma((3,)),
            dma((6,)),
            dma((6,)),
            dma((exchanges, 6)),
            dma((exchanges, 6)),
            dma((sums, nx * ny)),
            dma((sums, nx * ny)),
            dma((sums, nz)),
            dma((sums, nz)),
            dma((direct,)),
            dma((direct,)),
        ],
        compiler_params=pltpu.CompilerParams(
            collective_id=0, has_side_effects=True, vmem_limit_bytes=56 * 1024 * 1024
        ),
    )(target, maps, local_schur[0, 0, 0], inverse_rows[0, 0, 0])
    return (packed[None, None, None, :rhs], packed[rhs, :rhs])


def solution(mesh):
    placed = P("gx", "gy", "gz", None, None)
    sizes = (mesh.shape["gx"], mesh.shape["gy"], mesh.shape["gz"])
    return jax.shard_map(
        functools.partial(local, sizes),
        mesh=mesh,
        in_specs=(placed, placed, placed, placed),
        out_specs=(placed, P()),
        check_vma=False,
    )
```

```python
import functools

import jax
import jax.numpy as jnp
from jax import lax
from jax.experimental import pallas as pl
from jax.experimental.pallas import tpu as pltpu
from jax.sharding import PartitionSpec as P

ITERS = 3
EPSILON = 1e-06
MESH = pl.DeviceIdType.MESH
BF16 = jnp.bfloat16
F32 = jnp.float32
DIRECT_MAX = 32
PAIRED = (False, True, True)


def split(x):
    high = x.astype(BF16)
    low = (x - high.astype(F32)).astype(BF16)
    return jnp.concatenate([high, low], axis=0)


def merge(x):
    rows = x.shape[0] // 2
    return x[:rows] + x[rows:]


def mm(a, b):
    return jnp.dot(a, b, preferred_element_type=F32)


def rotate_column(column, section, cosines, sines, rhs_vec, triangle):
    column = list(column)
    for earlier in range(section):
        rotated_a = cosines[earlier] * column[earlier] + sines[earlier] * column[earlier + 1]
        rotated_b = -sines[earlier] * column[earlier] + cosines[earlier] * column[earlier + 1]
        column[earlier] = rotated_a
        column[earlier + 1] = rotated_b
    radius = jnp.sqrt(
        column[section] * column[section] + column[section + 1] * column[section + 1]
    )
    cosine = column[section] / radius
    sine_val = column[section + 1] / radius
    column[section] = radius
    cosines.append(cosine)
    sines.append(sine_val)
    rhs_vec[section + 1] = -sine_val * rhs_vec[section]
    rhs_vec[section] = cosine * rhs_vec[section]
    triangle.append(column[: section + 1])


def back_substitute(rhs_vec, triangle):
    num_cols = len(triangle)
    coeffs = [None] * num_cols
    for section in reversed(range(num_cols)):
        running = rhs_vec[section]
        for onward in range(section + 1, num_cols):
            running = running - triangle[onward][section] * coeffs[onward]
        coeffs[section] = running / triangle[section][section]
    return coeffs


class Axis:
    def __init__(self, axis, spot, size, own, face, at):
        self.axis = axis
        self.single = size == 2
        low, high = spot > 0, spot < size - 1
        if self.single:
            which = 2 * axis + jnp.where(low, 0, 1)
            self.faces = [(2 * axis, 2 * axis, which, None, jnp.where(low, -1, 1))]
            self.width = face
            self.start = pl.multiple_of(own + which * face, face)
        else:
            self.faces = [
                (2 * axis, 2 * axis + 1, 2 * axis, low, -1),
                (2 * axis + 1, 2 * axis, 2 * axis + 1, high, 1),
            ]
            self.width = 2 * face
            self.start = own + 2 * axis * face
        self.columns = pl.ds(self.start, self.width)
        self.packed = pl.ds(at, self.width)


def kernel(
    sizes, g_hbm, maps_hbm, k_hbm, b_hbm, out_ref,
    g_ref, maps_ref, k_ref, b_ref, near_maps, cols_ref, inverse_ref, send_buf, recv_buf, acc_ref,
    base_ref, t_ref, v_ref, z_ref, w_ref, last_ref, total_ref, plane_buf, line_buf, all_buf,
    weight_sem, map_send, map_recv, send_sem, recv_sem,
    plane_send, plane_recv, line_send, line_recv, all_send, all_recv,
):
    nx, ny, nz = sizes
    count = nx * ny * nz
    direct = count <= DIRECT_MAX
    rhs, own = g_ref.shape
    face = maps_ref.shape[-1]
    whole = k_ref.shape[0]
    ix, iy, iz = lax.axis_index("gx"), lax.axis_index("gy"), lax.axis_index("gz")
    here = (ix, iy, iz)

    groups = []
    at = 0
    for axis in range(3):
        if sizes[axis] > 1:
            groups.append(Axis(axis, here[axis], sizes[axis], own, face, at))
            at += groups[-1].width
    sending = [group for axis in (0, 2, 1) for group in groups if group.axis == axis]
    arriving = [group for axis in (1, 2, 0) for group in groups if group.axis == axis]
    final = arriving[-1]
    own_columns = pl.ds(0, own)

    def across(axis, step):
        place = list(here)
        place[axis] = place[axis] + step
        return tuple(place)

    def guarded(exists, body):
        if exists is None:
            body()
        else:
            pl.when(exists)(body)

    plane = [
        (lax.rem(ix + dx, nx), lax.rem(iy + dy, ny))
        for dx in range(nx) for dy in range(ny) if dx or dy
    ]
    line = [lax.rem(iz + dz, nz) for dz in range(1, nz)]
    others = [
        (lax.rem(ix + dx, nx), lax.rem(iy + dy, ny), lax.rem(iz + dz, nz))
        for dx in range(nx) for dy in range(ny) for dz in range(nz) if dx or dy or dz
    ]

    load_b = pltpu.make_async_copy(b_hbm, b_ref, weight_sem.at[0])
    load_own = pltpu.make_async_copy(
        k_hbm.at[pl.ds(0, own)], k_ref.at[pl.ds(0, own)], weight_sem.at[1]
    )
    ghosts = pl.ds(own, whole - own)
    load_ghosts = pltpu.make_async_copy(k_hbm.at[ghosts], k_ref.at[ghosts], weight_sem.at[2])
    load_g = pltpu.make_async_copy(g_hbm, g_ref, weight_sem.at[3])
    load_maps = pltpu.make_async_copy(maps_hbm, maps_ref, weight_sem.at[4])
    load_maps.start()
    load_g.start()
    load_b.start()

    barrier = pltpu.get_barrier_semaphore()
    greeted = [((px, py, iz), None) for px, py in plane]
    if nz <= 4:
        greeted += [
            (across(2, dz), iz + dz >= 0 if dz < 0 else iz + dz < nz)
            for dz in (-2, -1, 1, 2) if abs(dz) < nz
        ]
    else:
        greeted += [((ix, iy, pz), None) for pz in line]
    expected = 0
    for peer, exists in greeted:
        expected = expected + (1 if exists is None else exists.astype(jnp.int32))
        guarded(exists, lambda: pl.semaphore_signal(
            barrier, inc=1, device_id=peer, device_id_type=MESH
        ))

    cols_ref[...] = jnp.full(cols_ref.shape, -1, jnp.int32)
    v_ref[...] = jnp.zeros_like(v_ref)
    z_ref[...] = jnp.zeros_like(z_ref)
    w_ref[...] = jnp.zeros_like(w_ref)
    last_ref[...] = jnp.zeros_like(last_ref)
    total_ref[...] = jnp.zeros_like(total_ref)
    for group in groups:
        for slot, _, _, exists, _ in group.faces:
            if exists is not None:
                @pl.when(jnp.logical_not(exists))
                def _():
                    near_maps[slot] = jnp.full(near_maps.shape[1:], -1, jnp.int32)
                    for stage in range(3):
                        for j in range(ITERS):
                            recv_buf[stage, j, slot] = jnp.zeros(recv_buf.shape[3:], BF16)

    def map_copy(group, entry):
        slot, target, which, _, step = entry
        return pltpu.make_async_remote_copy(
            src_ref=maps_ref.at[which], dst_ref=near_maps.at[target],
            send_sem=map_send.at[slot], recv_sem=map_recv.at[target],
            device_id=across(group.axis, step), device_id_type=MESH,
        )

    def map_wait(group, entry):
        slot, _, which, _, step = entry
        return pltpu.make_async_remote_copy(
            src_ref=maps_ref.at[which], dst_ref=near_maps.at[slot],
            send_sem=map_send.at[slot], recv_sem=map_recv.at[slot],
            device_id=across(group.axis, step), device_id_type=MESH,
        )

    def height_of(stage):
        return pl.ds(0, 2 * rhs if PAIRED[stage] else rhs)

    def face_copy(stage, j, group, entry, arrival=False):
        slot, target, _, _, step = entry
        into = slot if arrival else target
        return pltpu.make_async_remote_copy(
            src_ref=send_buf.at[stage, j, slot, height_of(stage)],
            dst_ref=recv_buf.at[stage, j, into, height_of(stage)],
            send_sem=send_sem.at[stage, j, slot], recv_sem=recv_sem.at[stage, j, into],
            device_id=across(group.axis, step), device_id_type=MESH,
        )

    def plane_copy(r, peer, slot):
        mine = ix * ny + iy
        return pltpu.make_async_remote_copy(
            src_ref=plane_buf.at[r, mine], dst_ref=plane_buf.at[r, slot],
            send_sem=plane_send.at[r, peer[0] * ny + peer[1]], recv_sem=plane_recv.at[r, slot],
            device_id=(peer[0], peer[1], iz), device_id_type=MESH,
        )

    def line_copy(r, peer, slot):
        return pltpu.make_async_remote_copy(
            src_ref=line_buf.at[r, iz], dst_ref=line_buf.at[r, slot],
            send_sem=line_send.at[r, peer], recv_sem=line_recv.at[r, slot],
            device_id=(ix, iy, peer), device_id_type=MESH,
        )

    def rank(peer):
        return (peer[0] * ny + peer[1]) * nz + peer[2]

    def all_copy(peer, slot):
        return pltpu.make_async_remote_copy(
            src_ref=all_buf.at[rank(here)], dst_ref=all_buf.at[slot],
            send_sem=all_send.at[rank(peer)], recv_sem=all_recv.at[slot],
            device_id=peer, device_id_type=MESH,
        )

    lanes = lax.broadcasted_iota(jnp.int32, (rhs, 128), 1)
    rows = lax.broadcasted_iota(jnp.int32, (rhs, 128), 0)
    spread = 128 // rhs
    places = lax.rem(lanes, spread)
    mine = lax.div(lanes, spread) == rows

    def packed_sums():
        t = t_ref[...]
        last = last_ref[...]
        packed = jnp.where(places == ITERS, jnp.sum(t * t, axis=1, keepdims=True), 0.0)
        for k in range(ITERS):
            v = v_ref[k]
            packed = jnp.where(places == k, jnp.sum(v * t, axis=1, keepdims=True), packed)
            packed = jnp.where(
                places == ITERS + 1 + k, jnp.sum(v * last, axis=1, keepdims=True), packed
            )
        return jnp.sum(jnp.where(mine, packed, 0.0), axis=0, keepdims=True)

    def start_sums(r):
        plane_buf[r, ix * ny + iy] = packed_sums()
        for peer in plane:
            plane_copy(r, peer, ix * ny + iy).start()

    def pass_sums(r):
        for peer in plane:
            plane_copy(r, peer, peer[0] * ny + peer[1]).wait_recv()
        partial = plane_buf[r, 0]
        for at in range(1, nx * ny):
            partial = partial + plane_buf[r, at]
        line_buf[r, iz] = partial
        for peer in line:
            line_copy(r, peer, iz).start()

    def finish_sums(r):
        for peer in line:
            line_copy(r, peer, peer).wait_recv()
        total = line_buf[r, 0]
        for at in range(1, nz):
            total = total + line_buf[r, at]
        total_ref[r] = jnp.where(mine, total, 0.0)

    def pick(r, lane):
        return jnp.sum(jnp.where(places == lane, total_ref[r], 0.0), axis=1, keepdims=True)

    def heights(r, count):
        coeffs = [pick(r, k) for k in range(count)]
        running = pick(r, ITERS)
        for k in range(count):
            running = running - 2.0 * coeffs[k] * coeffs[k]
            for n in range(k + 1):
                element = coeffs[k] * pick(k + 1, ITERS + 1 + n) * coeffs[n]
                running = running + (element if n == k else 2.0 * element)
        return coeffs, jnp.sqrt(jnp.maximum(running, 0.0) + EPSILON)

    def arrived(stage, j, group):
        for entry in group.faces:
            guarded(entry[3], lambda: face_copy(stage, j, group, entry, True).wait_recv())
        blocks = [recv_buf[stage, j, entry[0], height_of(stage)] for entry in group.faces]
        return blocks[0] if len(blocks) == 1 else jnp.concatenate(blocks, axis=1)

    def joined(stage, product):
        return merge(product) if PAIRED[stage] else product

    def rounded(stage, values):
        return split(values) if PAIRED[stage] else values.astype(BF16)

    def take(values, index):
        sources = [values[:, at : at + 128] for at in range(0, values.shape[1], 128)]
        taken = []
        for at in range(0, index.shape[1], 128):
            spots = jnp.broadcast_to(index[:, at : at + 128], (rhs, 128))
            low = jnp.bitwise_and(spots, 127)
            high = jnp.right_shift(spots, 7)
            out = jnp.zeros((rhs, 128), F32)
            for k, source in enumerate(sources):
                picked = jnp.take_along_axis(source, low, axis=1, mode="promise_in_bounds")
                out = jnp.where(high == k, picked, out)
            taken.append(out)
        return jnp.concatenate(taken, axis=1)

    def scattered(stage, j, base):
        for group in arriving:
            for entry in group.faces:
                guarded(entry[3], lambda: face_copy(stage, j, group, entry, True).wait_recv())
                block = recv_buf[stage, j, entry[0], height_of(stage)].astype(F32)
                base = base + take(joined(stage, block), inverse_ref[entry[0]])
        return base

    def found(column, targets):
        order = lax.broadcasted_iota(jnp.int32, targets.shape, 0).astype(F32) + 1.0
        matched = jnp.where(column == targets, order, 0.0)
        return jnp.sum(matched, axis=0, keepdims=True).astype(jnp.int32) - 1

    def invert():
        for group in groups:
            for entry in group.faces:
                guarded(entry[3], lambda: map_wait(group, entry).wait_recv())
                cols_ref[pl.ds(entry[0], 1), :] = near_maps[entry[0]]
        turned = jnp.transpose(cols_ref[...].astype(F32))
        targets = lax.broadcasted_iota(jnp.int32, (face, own), 1).astype(F32)
        for group in groups:
            for slot, _, _, _, _ in group.faces:
                inverse_ref[slot] = found(turned[:, slot : slot + 1], targets)

    def send(stage, j, group, values):
        for at, entry in enumerate(group.faces):
            send_buf[stage, j, entry[0], height_of(stage)] = (
                values[:, at * face : (at + 1) * face]
            )

        def start(entry, when=None):
            exists = entry[3]
            if when is not None:
                exists = when if exists is None else jnp.logical_and(exists, when)
            guarded(exists, lambda: face_copy(stage, j, group, entry).start())

        if group is final and len(group.faces) == 2:
            odd = lax.rem(here[group.axis], 2) == 1
            start(group.faces[1], odd)
            start(group.faces[0])
            start(group.faces[1], jnp.logical_not(odd))
        else:
            for entry in group.faces:
                start(entry)

    def precondition(j, ready):
        pair = split(t_ref[...])
        first = True
        for group in sending:
            values = merge(mm(pair, b_ref[:, group.columns]))
            if first:
                ready()
                first = False
            send(0, j, group, rounded(0, values))
        base_ref[...] = merge(mm(pair, b_ref[:, own_columns]))

    def iteration(j, carry):
        start_sums(j)

        pl.when(j == 0)(invert)

        prepared = scattered(0, j, base_ref[...])
        pair = split(prepared)
        for group in sending:
            taken = [take(prepared, near_maps[entry[0]]) for entry in group.faces]
            values = taken[0] if len(taken) == 1 else jnp.concatenate(taken, axis=1)
            send(1, j, group, rounded(1, values))
        pass_sums(j)

        @pl.when(j == 0)
        def _():
            load_own.wait()

        targets = [group.columns for group in sending] + [own_columns]
        for columns in targets:
            acc_ref[:, columns] = merge(mm(pair, k_ref[own_columns, columns]))

        @pl.when(j == 0)
        def _():
            load_ghosts.wait()

        for group in arriving[:-1]:
            values = arrived(1, j, group)
            for columns in targets:
                acc_ref[:, columns] += joined(1, mm(values, k_ref[group.columns, columns]))
        values = arrived(1, j, final)

        def products(columns):
            product = mm(values, k_ref[final.columns, columns])
            return acc_ref[:, columns] + joined(1, product)

        for group in sending:
            send(2, j, group, rounded(2, products(group.columns)))
        base = products(own_columns)
        finish_sums(j)
        coeffs, height = heights(j, ITERS - 1)
        inverse = 1.0 / height
        newest = t_ref[...]
        for k in range(ITERS - 1):
            prepared = prepared - coeffs[k] * z_ref[k]
            newest = newest - coeffs[k] * v_ref[k]
        z_ref[j] = prepared * inverse
        newest = newest * inverse
        v_ref[j] = newest
        last_ref[...] = newest
        applied = scattered(2, j, base)
        for k in range(ITERS - 1):
            applied = applied - coeffs[k] * w_ref[k]
        applied = applied * inverse
        w_ref[j] = applied
        t_ref[...] = applied

        @pl.when(j < ITERS - 1)
        def _():
            precondition(j + 1, lambda: None)

        return carry

    def ready():
        load_own.start()
        load_ghosts.start()

    load_maps.wait()
    pl.semaphore_wait(barrier, expected)
    for group in groups:
        for entry in group.faces:
            guarded(entry[3], lambda: map_copy(group, entry).start())

    load_g.wait()
    t_ref[...] = g_ref[...]
    load_b.wait()
    precondition(0, ready)
    lax.fori_loop(0, ITERS, iteration, 0)
    if direct:
        all_buf[rank(here)] = packed_sums()
        for peer in others:
            all_copy(peer, rank(here)).start()
    else:
        start_sums(ITERS)
        pass_sums(ITERS)
    beta_norm = heights(0, 0)[1]
    rhs_vec = [beta_norm] + [jnp.zeros_like(beta_norm)] * ITERS
    cosines, sines, triangle = [], [], []
    for section in range(ITERS - 1):
        coeffs, height = heights(section + 1, section + 1)
        rotate_column(coeffs + [height], section, cosines, sines, rhs_vec, triangle)
    if direct:
        for peer in others:
            all_copy(peer, rank(peer)).wait_recv()
        total = jnp.sum(all_buf[...], axis=0)
        total_ref[ITERS] = jnp.where(mine, total, 0.0)
    else:
        finish_sums(ITERS)
    coeffs, height = heights(ITERS, ITERS)
    rotate_column(coeffs + [height], ITERS - 1, cosines, sines, rhs_vec, triangle)
    solved = back_substitute(rhs_vec, triangle)
    adjoint = solved[0] * z_ref[0]
    for k in range(1, ITERS):
        adjoint = adjoint + solved[k] * z_ref[k]
    out_ref[pl.ds(0, rhs), :] = adjoint
    ratio = jnp.abs(rhs_vec[ITERS]) / beta_norm
    ratio = jnp.sum(jnp.where(rows == lanes, ratio, 0.0), axis=0, keepdims=True)
    out_ref[pl.ds(rhs, 8), pl.ds(0, 128)] = jnp.broadcast_to(ratio, (8, 128))

    for group in groups:
        for entry in group.faces:
            def drain():
                map_copy(group, entry).wait_send()
                for stage in range(3):
                    for j in range(ITERS):
                        face_copy(stage, j, group, entry).wait_send()
            guarded(entry[3], drain)
    for r in range(ITERS if direct else ITERS + 1):
        for peer in plane:
            plane_copy(r, peer, ix * ny + iy).wait_send()
        for peer in line:
            line_copy(r, peer, iz).wait_send()
    if direct:
        for peer in others:
            all_copy(peer, rank(here)).wait_send()


def local(sizes, gradient, local_schur, inverse_rows, face_maps):
    nx, ny, nz = sizes
    target = gradient[0, 0, 0]
    rhs, own = target.shape
    maps = jnp.swapaxes(face_maps[0, 0], 0, 1)
    face = maps.shape[-1]
    whole = local_schur.shape[-1]
    sums = ITERS + 1
    count = nx * ny * nz
    direct = count if count <= DIRECT_MAX else 1
    vmem = pl.BlockSpec(memory_space=pltpu.VMEM)
    hbm = pl.BlockSpec(memory_space=pl.ANY)
    dma = pltpu.SemaphoreType.DMA
    packed = pl.pallas_call(
        functools.partial(kernel, sizes),
        out_shape=pltpu.VMEM((rhs + 8, own), F32),
        in_specs=[hbm, hbm, hbm, hbm],
        out_specs=vmem,
        scratch_shapes=[
            pltpu.VMEM((rhs, own), F32),
            pltpu.VMEM(maps.shape, jnp.int32),
            pltpu.VMEM((whole, whole), BF16),
            pltpu.VMEM((own, whole), BF16),
            pltpu.VMEM(maps.shape, jnp.int32),
            pltpu.VMEM((8, face), jnp.int32),
            pltpu.VMEM((6, 1, own), jnp.int32),
            pltpu.VMEM((3, ITERS, 6, 2 * rhs, face), BF16),
            pltpu.VMEM((3, ITERS, 6, 2 * rhs, face), BF16),
            pltpu.VMEM((rhs, whole), F32),
            pltpu.VMEM((rhs, own), F32),
            pltpu.VMEM((rhs, own), F32),
            pltpu.VMEM((ITERS, rhs, own), F32),
            pltpu.VMEM((ITERS, rhs, own), F32),
            pltpu.VMEM((ITERS, rhs, own), F32),
            pltpu.VMEM((rhs, own), F32),
            pltpu.VMEM((sums, rhs, 128), F32),
            pltpu.VMEM((sums, nx * ny, 1, 128), F32),
            pltpu.VMEM((sums, nz, 1, 128), F32),
            pltpu.VMEM((direct, 1, 128), F32),
            dma((5,)),
            dma((6,)),
            dma((6,)),
            dma((3, ITERS, 6)),
            dma((3, ITERS, 6)),
            dma((sums, nx * ny)),
            dma((sums, nx * ny)),
            dma((sums, nz)),
            dma((sums, nz)),
            dma((direct,)),
            dma((direct,)),
        ],
        compiler_params=pltpu.CompilerParams(
            collective_id=0, has_side_effects=True, vmem_limit_bytes=56 * 1024 * 1024
        ),
    )(target, maps, local_schur[0, 0, 0], inverse_rows[0, 0, 0])
    return (packed[None, None, None, :rhs], packed[rhs, :rhs])


def solution(mesh):
    placed = P("gx", "gy", "gz", None, None)
    sizes = (mesh.shape["gx"], mesh.shape["gy"], mesh.shape["gz"])
    return jax.shard_map(
        functools.partial(local, sizes),
        mesh=mesh,
        in_specs=(placed, placed, placed, placed),
        out_specs=(placed, P()),
        check_vma=False,
    )
```

```python
import functools

import jax
import jax.numpy as jnp
from jax import lax
from jax.experimental import pallas as pl
from jax.experimental.pallas import tpu as pltpu
from jax.sharding import PartitionSpec as P

ITERS = 3
EPSILON = 1e-06
MESH = pl.DeviceIdType.MESH
BF16 = jnp.bfloat16
F32 = jnp.float32
DIRECT_MAX = 32
PAIRED = (False, True, False)


def split(x):
    high = x.astype(BF16)
    low = (x - high.astype(F32)).astype(BF16)
    return jnp.concatenate([high, low], axis=0)


def merge(x):
    rows = x.shape[0] // 2
    return x[:rows] + x[rows:]


def mm(a, b):
    return jnp.dot(a, b, preferred_element_type=F32)


def rotate_column(column, section, cosines, sines, rhs_vec, triangle):
    column = list(column)
    for earlier in range(section):
        rotated_a = cosines[earlier] * column[earlier] + sines[earlier] * column[earlier + 1]
        rotated_b = -sines[earlier] * column[earlier] + cosines[earlier] * column[earlier + 1]
        column[earlier] = rotated_a
        column[earlier + 1] = rotated_b
    radius = jnp.sqrt(
        column[section] * column[section] + column[section + 1] * column[section + 1]
    )
    cosine = column[section] / radius
    sine_val = column[section + 1] / radius
    column[section] = radius
    cosines.append(cosine)
    sines.append(sine_val)
    rhs_vec[section + 1] = -sine_val * rhs_vec[section]
    rhs_vec[section] = cosine * rhs_vec[section]
    triangle.append(column[: section + 1])


def back_substitute(rhs_vec, triangle):
    num_cols = len(triangle)
    coeffs = [None] * num_cols
    for section in reversed(range(num_cols)):
        running = rhs_vec[section]
        for onward in range(section + 1, num_cols):
            running = running - triangle[onward][section] * coeffs[onward]
        coeffs[section] = running / triangle[section][section]
    return coeffs


class Axis:
    def __init__(self, axis, spot, size, own, face, at):
        self.axis = axis
        self.single = size == 2
        low, high = spot > 0, spot < size - 1
        if self.single:
            which = 2 * axis + jnp.where(low, 0, 1)
            self.faces = [(2 * axis, 2 * axis, which, None, jnp.where(low, -1, 1))]
            self.width = face
            self.start = pl.multiple_of(own + which * face, face)
        else:
            self.faces = [
                (2 * axis, 2 * axis + 1, 2 * axis, low, -1),
                (2 * axis + 1, 2 * axis, 2 * axis + 1, high, 1),
            ]
            self.width = 2 * face
            self.start = own + 2 * axis * face
        self.columns = pl.ds(self.start, self.width)
        self.packed = pl.ds(at, self.width)


def kernel(
    sizes, g_hbm, maps_hbm, k_hbm, b_hbm, out_ref,
    g_ref, maps_ref, k_ref, b_ref, near_maps, cols_ref, inverse_ref, send_buf, recv_buf, acc_ref,
    base_ref, t_ref, v_ref, z_ref, w_ref, last_ref, total_ref, plane_buf, line_buf, all_buf,
    weight_sem, map_send, map_recv, send_sem, recv_sem,
    plane_send, plane_recv, line_send, line_recv, all_send, all_recv,
):
    nx, ny, nz = sizes
    count = nx * ny * nz
    direct = count <= DIRECT_MAX
    rhs, own = g_ref.shape
    face = maps_ref.shape[-1]
    whole = k_ref.shape[0]
    ix, iy, iz = lax.axis_index("gx"), lax.axis_index("gy"), lax.axis_index("gz")
    here = (ix, iy, iz)

    groups = []
    at = 0
    for axis in range(3):
        if sizes[axis] > 1:
            groups.append(Axis(axis, here[axis], sizes[axis], own, face, at))
            at += groups[-1].width
    sending = [group for axis in (0, 2, 1) for group in groups if group.axis == axis]
    arriving = [group for axis in (1, 2, 0) for group in groups if group.axis == axis]
    final = arriving[-1]
    own_columns = pl.ds(0, own)

    def across(axis, step):
        place = list(here)
        place[axis] = place[axis] + step
        return tuple(place)

    def guarded(exists, body):
        if exists is None:
            body()
        else:
            pl.when(exists)(body)

    plane = [
        (lax.rem(ix + dx, nx), lax.rem(iy + dy, ny))
        for dx in range(nx) for dy in range(ny) if dx or dy
    ]
    line = [lax.rem(iz + dz, nz) for dz in range(1, nz)]
    others = [
        (lax.rem(ix + dx, nx), lax.rem(iy + dy, ny), lax.rem(iz + dz, nz))
        for dx in range(nx) for dy in range(ny) for dz in range(nz) if dx or dy or dz
    ]

    load_b = pltpu.make_async_copy(b_hbm, b_ref, weight_sem.at[0])
    load_own = pltpu.make_async_copy(
        k_hbm.at[pl.ds(0, own)], k_ref.at[pl.ds(0, own)], weight_sem.at[1]
    )
    ghosts = pl.ds(own, whole - own)
    load_ghosts = pltpu.make_async_copy(k_hbm.at[ghosts], k_ref.at[ghosts], weight_sem.at[2])
    load_g = pltpu.make_async_copy(g_hbm, g_ref, weight_sem.at[3])
    load_maps = pltpu.make_async_copy(maps_hbm, maps_ref, weight_sem.at[4])
    load_maps.start()
    load_g.start()
    load_b.start()

    barrier = pltpu.get_barrier_semaphore()
    greeted = [((px, py, iz), None) for px, py in plane]
    if nz <= 4:
        greeted += [
            (across(2, dz), iz + dz >= 0 if dz < 0 else iz + dz < nz)
            for dz in (-2, -1, 1, 2) if abs(dz) < nz
        ]
    else:
        greeted += [((ix, iy, pz), None) for pz in line]
    expected = 0
    for peer, exists in greeted:
        expected = expected + (1 if exists is None else exists.astype(jnp.int32))
        guarded(exists, lambda: pl.semaphore_signal(
            barrier, inc=1, device_id=peer, device_id_type=MESH
        ))

    cols_ref[...] = jnp.full(cols_ref.shape, -1, jnp.int32)
    v_ref[...] = jnp.zeros_like(v_ref)
    z_ref[...] = jnp.zeros_like(z_ref)
    w_ref[...] = jnp.zeros_like(w_ref)
    last_ref[...] = jnp.zeros_like(last_ref)
    total_ref[...] = jnp.zeros_like(total_ref)
    for group in groups:
        for slot, _, _, exists, _ in group.faces:
            if exists is not None:
                @pl.when(jnp.logical_not(exists))
                def _():
                    near_maps[slot] = jnp.full(near_maps.shape[1:], -1, jnp.int32)
                    for stage in range(3):
                        for j in range(ITERS):
                            recv_buf[stage, j, slot] = jnp.zeros(recv_buf.shape[3:], BF16)

    def map_copy(group, entry):
        slot, target, which, _, step = entry
        return pltpu.make_async_remote_copy(
            src_ref=maps_ref.at[which], dst_ref=near_maps.at[target],
            send_sem=map_send.at[slot], recv_sem=map_recv.at[target],
            device_id=across(group.axis, step), device_id_type=MESH,
        )

    def map_wait(group, entry):
        slot, _, which, _, step = entry
        return pltpu.make_async_remote_copy(
            src_ref=maps_ref.at[which], dst_ref=near_maps.at[slot],
            send_sem=map_send.at[slot], recv_sem=map_recv.at[slot],
            device_id=across(group.axis, step), device_id_type=MESH,
        )

    def height_of(stage):
        return pl.ds(0, 2 * rhs if PAIRED[stage] else rhs)

    def face_copy(stage, j, group, entry, arrival=False):
        slot, target, _, _, step = entry
        into = slot if arrival else target
        return pltpu.make_async_remote_copy(
            src_ref=send_buf.at[stage, j, slot, height_of(stage)],
            dst_ref=recv_buf.at[stage, j, into, height_of(stage)],
            send_sem=send_sem.at[stage, j, slot], recv_sem=recv_sem.at[stage, j, into],
            device_id=across(group.axis, step), device_id_type=MESH,
        )

    def plane_copy(r, peer, slot):
        mine = ix * ny + iy
        return pltpu.make_async_remote_copy(
            src_ref=plane_buf.at[r, mine], dst_ref=plane_buf.at[r, slot],
            send_sem=plane_send.at[r, peer[0] * ny + peer[1]], recv_sem=plane_recv.at[r, slot],
            device_id=(peer[0], peer[1], iz), device_id_type=MESH,
        )

    def line_copy(r, peer, slot):
        return pltpu.make_async_remote_copy(
            src_ref=line_buf.at[r, iz], dst_ref=line_buf.at[r, slot],
            send_sem=line_send.at[r, peer], recv_sem=line_recv.at[r, slot],
            device_id=(ix, iy, peer), device_id_type=MESH,
        )

    def rank(peer):
        return (peer[0] * ny + peer[1]) * nz + peer[2]

    def all_copy(peer, slot):
        return pltpu.make_async_remote_copy(
            src_ref=all_buf.at[rank(here)], dst_ref=all_buf.at[slot],
            send_sem=all_send.at[rank(peer)], recv_sem=all_recv.at[slot],
            device_id=peer, device_id_type=MESH,
        )

    lanes = lax.broadcasted_iota(jnp.int32, (rhs, 128), 1)
    rows = lax.broadcasted_iota(jnp.int32, (rhs, 128), 0)
    spread = 128 // rhs
    places = lax.rem(lanes, spread)
    mine = lax.div(lanes, spread) == rows

    def packed_sums():
        t = t_ref[...]
        last = last_ref[...]
        packed = jnp.where(places == ITERS, jnp.sum(t * t, axis=1, keepdims=True), 0.0)
        for k in range(ITERS):
            v = v_ref[k]
            packed = jnp.where(places == k, jnp.sum(v * t, axis=1, keepdims=True), packed)
            packed = jnp.where(
                places == ITERS + 1 + k, jnp.sum(v * last, axis=1, keepdims=True), packed
            )
        return jnp.sum(jnp.where(mine, packed, 0.0), axis=0, keepdims=True)

    def start_sums(r):
        plane_buf[r, ix * ny + iy] = packed_sums()
        for peer in plane:
            plane_copy(r, peer, ix * ny + iy).start()

    def pass_sums(r):
        for peer in plane:
            plane_copy(r, peer, peer[0] * ny + peer[1]).wait_recv()
        partial = plane_buf[r, 0]
        for at in range(1, nx * ny):
            partial = partial + plane_buf[r, at]
        line_buf[r, iz] = partial
        for peer in line:
            line_copy(r, peer, iz).start()

    def finish_sums(r):
        for peer in line:
            line_copy(r, peer, peer).wait_recv()
        total = line_buf[r, 0]
        for at in range(1, nz):
            total = total + line_buf[r, at]
        total_ref[r] = jnp.where(mine, total, 0.0)

    def pick(r, lane):
        return jnp.sum(jnp.where(places == lane, total_ref[r], 0.0), axis=1, keepdims=True)

    def heights(r, count):
        coeffs = [pick(r, k) for k in range(count)]
        running = pick(r, ITERS)
        for k in range(count):
            running = running - 2.0 * coeffs[k] * coeffs[k]
            for n in range(k + 1):
                element = coeffs[k] * pick(k + 1, ITERS + 1 + n) * coeffs[n]
                running = running + (element if n == k else 2.0 * element)
        return coeffs, jnp.sqrt(jnp.maximum(running, 0.0) + EPSILON)

    def arrived(stage, j, group):
        for entry in group.faces:
            guarded(entry[3], lambda: face_copy(stage, j, group, entry, True).wait_recv())
        blocks = [recv_buf[stage, j, entry[0], height_of(stage)] for entry in group.faces]
        return blocks[0] if len(blocks) == 1 else jnp.concatenate(blocks, axis=1)

    def joined(stage, product):
        return merge(product) if PAIRED[stage] else product

    def rounded(stage, values):
        return split(values) if PAIRED[stage] else values.astype(BF16)

    def take(values, index):
        sources = [values[:, at : at + 128] for at in range(0, values.shape[1], 128)]
        taken = []
        for at in range(0, index.shape[1], 128):
            spots = jnp.broadcast_to(index[:, at : at + 128], (rhs, 128))
            low = jnp.bitwise_and(spots, 127)
            high = jnp.right_shift(spots, 7)
            out = jnp.zeros((rhs, 128), F32)
            for k, source in enumerate(sources):
                picked = jnp.take_along_axis(source, low, axis=1, mode="promise_in_bounds")
                out = jnp.where(high == k, picked, out)
            taken.append(out)
        return jnp.concatenate(taken, axis=1)

    def scattered(stage, j, base):
        for group in arriving:
            for entry in group.faces:
                guarded(entry[3], lambda: face_copy(stage, j, group, entry, True).wait_recv())
                block = recv_buf[stage, j, entry[0], height_of(stage)].astype(F32)
                base = base + take(joined(stage, block), inverse_ref[entry[0]])
        return base

    def found(column, targets):
        order = lax.broadcasted_iota(jnp.int32, targets.shape, 0).astype(F32) + 1.0
        matched = jnp.where(column == targets, order, 0.0)
        return jnp.sum(matched, axis=0, keepdims=True).astype(jnp.int32) - 1

    def invert():
        for group in groups:
            for entry in group.faces:
                guarded(entry[3], lambda: map_wait(group, entry).wait_recv())
                cols_ref[pl.ds(entry[0], 1), :] = near_maps[entry[0]]
        turned = jnp.transpose(cols_ref[...].astype(F32))
        targets = lax.broadcasted_iota(jnp.int32, (face, own), 1).astype(F32)
        for group in groups:
            for slot, _, _, _, _ in group.faces:
                inverse_ref[slot] = found(turned[:, slot : slot + 1], targets)

    def send(stage, j, group, values):
        for at, entry in enumerate(group.faces):
            send_buf[stage, j, entry[0], height_of(stage)] = (
                values[:, at * face : (at + 1) * face]
            )

        def start(entry, when=None):
            exists = entry[3]
            if when is not None:
                exists = when if exists is None else jnp.logical_and(exists, when)
            guarded(exists, lambda: face_copy(stage, j, group, entry).start())

        if group is final and len(group.faces) == 2:
            odd = lax.rem(here[group.axis], 2) == 1
            start(group.faces[1], odd)
            start(group.faces[0])
            start(group.faces[1], jnp.logical_not(odd))
        else:
            for entry in group.faces:
                start(entry)

    def precondition(j, ready):
        pair = split(t_ref[...])
        first = True
        for group in sending:
            values = merge(mm(pair, b_ref[:, group.columns]))
            if first:
                ready()
                first = False
            send(0, j, group, rounded(0, values))
        base_ref[...] = merge(mm(pair, b_ref[:, own_columns]))

    def iteration(j, carry):
        start_sums(j)

        pl.when(j == 0)(invert)

        prepared = scattered(0, j, base_ref[...])
        pair = split(prepared)
        for group in sending:
            taken = [take(prepared, near_maps[entry[0]]) for entry in group.faces]
            values = taken[0] if len(taken) == 1 else jnp.concatenate(taken, axis=1)
            send(1, j, group, rounded(1, values))
        pass_sums(j)

        @pl.when(j == 0)
        def _():
            load_own.wait()

        targets = [group.columns for group in sending] + [own_columns]
        for columns in targets:
            acc_ref[:, columns] = merge(mm(pair, k_ref[own_columns, columns]))

        @pl.when(j == 0)
        def _():
            load_ghosts.wait()

        for group in arriving[:-1]:
            values = arrived(1, j, group)
            for columns in targets:
                acc_ref[:, columns] += joined(1, mm(values, k_ref[group.columns, columns]))
        values = arrived(1, j, final)

        def products(columns):
            product = mm(values, k_ref[final.columns, columns])
            return acc_ref[:, columns] + joined(1, product)

        for group in sending:
            send(2, j, group, rounded(2, products(group.columns)))
        base = products(own_columns)
        finish_sums(j)
        coeffs, height = heights(j, ITERS - 1)
        inverse = 1.0 / height
        newest = t_ref[...]
        for k in range(ITERS - 1):
            prepared = prepared - coeffs[k] * z_ref[k]
            newest = newest - coeffs[k] * v_ref[k]
        z_ref[j] = prepared * inverse
        newest = newest * inverse
        v_ref[j] = newest
        last_ref[...] = newest
        applied = scattered(2, j, base)
        for k in range(ITERS - 1):
            applied = applied - coeffs[k] * w_ref[k]
        applied = applied * inverse
        w_ref[j] = applied
        t_ref[...] = applied

        @pl.when(j < ITERS - 1)
        def _():
            precondition(j + 1, lambda: None)

        return carry

    def ready():
        load_own.start()
        load_ghosts.start()

    load_maps.wait()
    pl.semaphore_wait(barrier, expected)
    for group in groups:
        for entry in group.faces:
            guarded(entry[3], lambda: map_copy(group, entry).start())

    load_g.wait()
    t_ref[...] = g_ref[...]
    load_b.wait()
    precondition(0, ready)
    lax.fori_loop(0, ITERS, iteration, 0)
    if direct:
        all_buf[rank(here)] = packed_sums()
        for peer in others:
            all_copy(peer, rank(here)).start()
    else:
        start_sums(ITERS)
        pass_sums(ITERS)
    beta_norm = heights(0, 0)[1]
    rhs_vec = [beta_norm] + [jnp.zeros_like(beta_norm)] * ITERS
    cosines, sines, triangle = [], [], []
    for section in range(ITERS - 1):
        coeffs, height = heights(section + 1, section + 1)
        rotate_column(coeffs + [height], section, cosines, sines, rhs_vec, triangle)
    for group in groups:
        for entry in group.faces:
            def drain():
                map_copy(group, entry).wait_send()
                for stage in range(3):
                    for j in range(ITERS):
                        face_copy(stage, j, group, entry).wait_send()
            guarded(entry[3], drain)
    for r in range(ITERS if direct else ITERS + 1):
        for peer in plane:
            plane_copy(r, peer, ix * ny + iy).wait_send()
        for peer in line:
            line_copy(r, peer, iz).wait_send()
    if direct:
        for peer in others:
            all_copy(peer, rank(here)).wait_send()
        for peer in others:
            all_copy(peer, rank(peer)).wait_recv()
        total = jnp.sum(all_buf[...], axis=0)
        total_ref[ITERS] = jnp.where(mine, total, 0.0)
    else:
        finish_sums(ITERS)
    coeffs, height = heights(ITERS, ITERS)
    rotate_column(coeffs + [height], ITERS - 1, cosines, sines, rhs_vec, triangle)
    solved = back_substitute(rhs_vec, triangle)
    adjoint = solved[0] * z_ref[0]
    for k in range(1, ITERS):
        adjoint = adjoint + solved[k] * z_ref[k]
    out_ref[pl.ds(0, rhs), :] = adjoint
    ratio = jnp.abs(rhs_vec[ITERS]) / beta_norm
    ratio = jnp.sum(jnp.where(rows == lanes, ratio, 0.0), axis=0, keepdims=True)
    out_ref[pl.ds(rhs, 8), pl.ds(0, 128)] = jnp.broadcast_to(ratio, (8, 128))


def local(sizes, gradient, local_schur, inverse_rows, face_maps):
    nx, ny, nz = sizes
    target = gradient[0, 0, 0]
    rhs, own = target.shape
    maps = jnp.swapaxes(face_maps[0, 0], 0, 1)
    face = maps.shape[-1]
    whole = local_schur.shape[-1]
    sums = ITERS + 1
    count = nx * ny * nz
    direct = count if count <= DIRECT_MAX else 1
    vmem = pl.BlockSpec(memory_space=pltpu.VMEM)
    hbm = pl.BlockSpec(memory_space=pl.ANY)
    dma = pltpu.SemaphoreType.DMA
    packed = pl.pallas_call(
        functools.partial(kernel, sizes),
        out_shape=pltpu.VMEM((rhs + 8, own), F32),
        in_specs=[hbm, hbm, hbm, hbm],
        out_specs=vmem,
        scratch_shapes=[
            pltpu.VMEM((rhs, own), F32),
            pltpu.VMEM(maps.shape, jnp.int32),
            pltpu.VMEM((whole, whole), BF16),
            pltpu.VMEM((own, whole), BF16),
            pltpu.VMEM(maps.shape, jnp.int32),
            pltpu.VMEM((8, face), jnp.int32),
            pltpu.VMEM((6, 1, own), jnp.int32),
            pltpu.VMEM((3, ITERS, 6, 2 * rhs, face), BF16),
            pltpu.VMEM((3, ITERS, 6, 2 * rhs, face), BF16),
            pltpu.VMEM((rhs, whole), F32),
            pltpu.VMEM((rhs, own), F32),
            pltpu.VMEM((rhs, own), F32),
            pltpu.VMEM((ITERS, rhs, own), F32),
            pltpu.VMEM((ITERS, rhs, own), F32),
            pltpu.VMEM((ITERS, rhs, own), F32),
            pltpu.VMEM((rhs, own), F32),
            pltpu.VMEM((sums, rhs, 128), F32),
            pltpu.VMEM((sums, nx * ny, 1, 128), F32),
            pltpu.VMEM((sums, nz, 1, 128), F32),
            pltpu.VMEM((direct, 1, 128), F32),
            dma((5,)),
            dma((6,)),
            dma((6,)),
            dma((3, ITERS, 6)),
            dma((3, ITERS, 6)),
            dma((sums, nx * ny)),
            dma((sums, nx * ny)),
            dma((sums, nz)),
            dma((sums, nz)),
            dma((direct,)),
            dma((direct,)),
        ],
        compiler_params=pltpu.CompilerParams(
            collective_id=0, has_side_effects=True, vmem_limit_bytes=56 * 1024 * 1024
        ),
    )(target, maps, local_schur[0, 0, 0], inverse_rows[0, 0, 0])
    return (packed[None, None, None, :rhs], packed[rhs, :rhs])


def solution(mesh):
    placed = P("gx", "gy", "gz", None, None)
    sizes = (mesh.shape["gx"], mesh.shape["gy"], mesh.shape["gz"])
    return jax.shard_map(
        functools.partial(local, sizes),
        mesh=mesh,
        in_specs=(placed, placed, placed, placed),
        out_specs=(placed, P()),
        check_vma=False,
    )
```

```python
import functools

import jax
import jax.numpy as jnp
from jax import lax
from jax.experimental import pallas as pl
from jax.experimental.pallas import tpu as pltpu
from jax.sharding import PartitionSpec as P

ITERS = 3
EPSILON = 1e-06
MESH = pl.DeviceIdType.MESH
BF16 = jnp.bfloat16
F32 = jnp.float32
DIRECT_MAX = 32
PAIRED = (False, True, False)


def split(x):
    high = x.astype(BF16)
    low = (x - high.astype(F32)).astype(BF16)
    return jnp.concatenate([high, low], axis=0)


def merge(x):
    rows = x.shape[0] // 2
    return x[:rows] + x[rows:]


def mm(a, b):
    return jnp.dot(a, b, preferred_element_type=F32)


def rotate_column(column, section, cosines, sines, rhs_vec, triangle):
    column = list(column)
    for earlier in range(section):
        rotated_a = cosines[earlier] * column[earlier] + sines[earlier] * column[earlier + 1]
        rotated_b = -sines[earlier] * column[earlier] + cosines[earlier] * column[earlier + 1]
        column[earlier] = rotated_a
        column[earlier + 1] = rotated_b
    radius = jnp.sqrt(
        column[section] * column[section] + column[section + 1] * column[section + 1]
    )
    cosine = column[section] / radius
    sine_val = column[section + 1] / radius
    column[section] = radius
    cosines.append(cosine)
    sines.append(sine_val)
    rhs_vec[section + 1] = -sine_val * rhs_vec[section]
    rhs_vec[section] = cosine * rhs_vec[section]
    triangle.append(column[: section + 1])


def back_substitute(rhs_vec, triangle):
    num_cols = len(triangle)
    coeffs = [None] * num_cols
    for section in reversed(range(num_cols)):
        running = rhs_vec[section]
        for onward in range(section + 1, num_cols):
            running = running - triangle[onward][section] * coeffs[onward]
        coeffs[section] = running / triangle[section][section]
    return coeffs


class Axis:
    def __init__(self, axis, spot, size, own, face, at):
        self.axis = axis
        self.single = size == 2
        low, high = spot > 0, spot < size - 1
        if self.single:
            which = 2 * axis + jnp.where(low, 0, 1)
            self.faces = [(2 * axis, 2 * axis, which, None, jnp.where(low, -1, 1))]
            self.width = face
            self.start = pl.multiple_of(own + which * face, face)
        else:
            self.faces = [
                (2 * axis, 2 * axis + 1, 2 * axis, low, -1),
                (2 * axis + 1, 2 * axis, 2 * axis + 1, high, 1),
            ]
            self.width = 2 * face
            self.start = own + 2 * axis * face
        self.columns = pl.ds(self.start, self.width)
        self.packed = pl.ds(at, self.width)


def kernel(
    sizes, g_hbm, maps_hbm, k_hbm, b_hbm, out_ref,
    g_ref, maps_ref, k_ref, b_ref, near_maps, cols_ref, inverse_ref, send_buf, recv_buf, acc_ref,
    base_ref, t_ref, v_ref, z_ref, w_ref, last_ref, total_ref, plane_buf, line_buf, all_buf,
    weight_sem, map_send, map_recv, send_sem, recv_sem,
    plane_send, plane_recv, line_send, line_recv, all_send, all_recv,
):
    nx, ny, nz = sizes
    count = nx * ny * nz
    direct = count <= DIRECT_MAX
    rhs, own = g_ref.shape
    face = maps_ref.shape[-1]
    whole = k_ref.shape[0]
    ix, iy, iz = lax.axis_index("gx"), lax.axis_index("gy"), lax.axis_index("gz")
    here = (ix, iy, iz)

    groups = []
    at = 0
    for axis in range(3):
        if sizes[axis] > 1:
            groups.append(Axis(axis, here[axis], sizes[axis], own, face, at))
            at += groups[-1].width
    sending = [group for axis in (0, 2, 1) for group in groups if group.axis == axis]
    arriving = [group for axis in (1, 2, 0) for group in groups if group.axis == axis]
    final = arriving[-1]
    own_columns = pl.ds(0, own)

    def across(axis, step):
        place = list(here)
        place[axis] = place[axis] + step
        return tuple(place)

    def guarded(exists, body):
        if exists is None:
            body()
        else:
            pl.when(exists)(body)

    plane = [
        (lax.rem(ix + dx, nx), lax.rem(iy + dy, ny))
        for dx in range(nx) for dy in range(ny) if dx or dy
    ]
    line = [lax.rem(iz + dz, nz) for dz in range(1, nz)]
    others = [
        (lax.rem(ix + dx, nx), lax.rem(iy + dy, ny), lax.rem(iz + dz, nz))
        for dx in range(nx) for dy in range(ny) for dz in range(nz) if dx or dy or dz
    ]

    load_b = pltpu.make_async_copy(b_hbm, b_ref, weight_sem.at[0])
    load_own = pltpu.make_async_copy(
        k_hbm.at[pl.ds(0, own)], k_ref.at[pl.ds(0, own)], weight_sem.at[1]
    )
    ghosts = pl.ds(own, whole - own)
    load_ghosts = pltpu.make_async_copy(k_hbm.at[ghosts], k_ref.at[ghosts], weight_sem.at[2])
    load_g = pltpu.make_async_copy(g_hbm, g_ref, weight_sem.at[3])
    load_maps = pltpu.make_async_copy(maps_hbm, maps_ref, weight_sem.at[4])
    load_maps.start()
    load_g.start()
    load_b.start()

    barrier = pltpu.get_barrier_semaphore()
    greeted = [((px, py, iz), None) for px, py in plane]
    if nz <= 4:
        greeted += [
            (across(2, dz), iz + dz >= 0 if dz < 0 else iz + dz < nz)
            for dz in (-2, -1, 1, 2) if abs(dz) < nz
        ]
    else:
        greeted += [((ix, iy, pz), None) for pz in line]
    expected = 0
    for peer, exists in greeted:
        expected = expected + (1 if exists is None else exists.astype(jnp.int32))
        guarded(exists, lambda: pl.semaphore_signal(
            barrier, inc=1, device_id=peer, device_id_type=MESH
        ))

    cols_ref[...] = jnp.full(cols_ref.shape, -1, jnp.int32)
    v_ref[...] = jnp.zeros_like(v_ref)
    z_ref[...] = jnp.zeros_like(z_ref)
    w_ref[...] = jnp.zeros_like(w_ref)
    last_ref[...] = jnp.zeros_like(last_ref)
    total_ref[...] = jnp.zeros_like(total_ref)
    for group in groups:
        for slot, _, _, exists, _ in group.faces:
            if exists is not None:
                @pl.when(jnp.logical_not(exists))
                def _():
                    near_maps[slot] = jnp.full(near_maps.shape[1:], -1, jnp.int32)
                    for stage in range(3):
                        for j in range(ITERS):
                            recv_buf[stage, j, slot] = jnp.zeros(recv_buf.shape[3:], BF16)

    def map_copy(group, entry):
        slot, target, which, _, step = entry
        return pltpu.make_async_remote_copy(
            src_ref=maps_ref.at[which], dst_ref=near_maps.at[target],
            send_sem=map_send.at[slot], recv_sem=map_recv.at[target],
            device_id=across(group.axis, step), device_id_type=MESH,
        )

    def map_wait(group, entry):
        slot, _, which, _, step = entry
        return pltpu.make_async_remote_copy(
            src_ref=maps_ref.at[which], dst_ref=near_maps.at[slot],
            send_sem=map_send.at[slot], recv_sem=map_recv.at[slot],
            device_id=across(group.axis, step), device_id_type=MESH,
        )

    def height_of(stage):
        return pl.ds(0, 2 * rhs if PAIRED[stage] else rhs)

    def face_copy(stage, j, group, entry, arrival=False):
        slot, target, _, _, step = entry
        into = slot if arrival else target
        return pltpu.make_async_remote_copy(
            src_ref=send_buf.at[stage, j, slot, height_of(stage)],
            dst_ref=recv_buf.at[stage, j, into, height_of(stage)],
            send_sem=send_sem.at[stage, j, slot], recv_sem=recv_sem.at[stage, j, into],
            device_id=across(group.axis, step), device_id_type=MESH,
        )

    def plane_copy(r, peer, slot):
        mine = ix * ny + iy
        return pltpu.make_async_remote_copy(
            src_ref=plane_buf.at[r, mine], dst_ref=plane_buf.at[r, slot],
            send_sem=plane_send.at[r, peer[0] * ny + peer[1]], recv_sem=plane_recv.at[r, slot],
            device_id=(peer[0], peer[1], iz), device_id_type=MESH,
        )

    def line_copy(r, peer, slot):
        return pltpu.make_async_remote_copy(
            src_ref=line_buf.at[r, iz], dst_ref=line_buf.at[r, slot],
            send_sem=line_send.at[r, peer], recv_sem=line_recv.at[r, slot],
            device_id=(ix, iy, peer), device_id_type=MESH,
        )

    def rank(peer):
        return (peer[0] * ny + peer[1]) * nz + peer[2]

    def all_copy(peer, slot):
        return pltpu.make_async_remote_copy(
            src_ref=all_buf.at[rank(here)], dst_ref=all_buf.at[slot],
            send_sem=all_send.at[rank(peer)], recv_sem=all_recv.at[slot],
            device_id=peer, device_id_type=MESH,
        )

    lanes = lax.broadcasted_iota(jnp.int32, (rhs, 128), 1)
    rows = lax.broadcasted_iota(jnp.int32, (rhs, 128), 0)
    spread = 128 // rhs
    places = lax.rem(lanes, spread)
    mine = lax.div(lanes, spread) == rows

    def packed_sums():
        t = t_ref[...]
        last = last_ref[...]
        packed = jnp.where(places == ITERS, jnp.sum(t * t, axis=1, keepdims=True), 0.0)
        for k in range(ITERS):
            v = v_ref[k]
            packed = jnp.where(places == k, jnp.sum(v * t, axis=1, keepdims=True), packed)
            packed = jnp.where(
                places == ITERS + 1 + k, jnp.sum(v * last, axis=1, keepdims=True), packed
            )
        return jnp.sum(jnp.where(mine, packed, 0.0), axis=0, keepdims=True)

    def start_sums(r):
        plane_buf[r, ix * ny + iy] = packed_sums()
        for peer in plane:
            plane_copy(r, peer, ix * ny + iy).start()

    def pass_sums(r):
        for peer in plane:
            plane_copy(r, peer, peer[0] * ny + peer[1]).wait_recv()
        partial = plane_buf[r, 0]
        for at in range(1, nx * ny):
            partial = partial + plane_buf[r, at]
        line_buf[r, iz] = partial
        for peer in line:
            line_copy(r, peer, iz).start()

    def finish_sums(r):
        for peer in line:
            line_copy(r, peer, peer).wait_recv()
        total = line_buf[r, 0]
        for at in range(1, nz):
            total = total + line_buf[r, at]
        total_ref[r] = jnp.where(mine, total, 0.0)

    def pick(r, lane):
        return jnp.sum(jnp.where(places == lane, total_ref[r], 0.0), axis=1, keepdims=True)

    def heights(r, count):
        coeffs = [pick(r, k) for k in range(count)]
        running = pick(r, ITERS)
        for k in range(count):
            running = running - 2.0 * coeffs[k] * coeffs[k]
            for n in range(k + 1):
                element = coeffs[k] * pick(k + 1, ITERS + 1 + n) * coeffs[n]
                running = running + (element if n == k else 2.0 * element)
        return coeffs, jnp.sqrt(jnp.maximum(running, 0.0) + EPSILON)

    def arrived(stage, j, group):
        for entry in group.faces:
            guarded(entry[3], lambda: face_copy(stage, j, group, entry, True).wait_recv())
        blocks = [recv_buf[stage, j, entry[0], height_of(stage)] for entry in group.faces]
        return blocks[0] if len(blocks) == 1 else jnp.concatenate(blocks, axis=1)

    def joined(stage, product):
        return merge(product) if PAIRED[stage] else product

    def rounded(stage, values):
        return split(values) if PAIRED[stage] else values.astype(BF16)

    def take(values, index):
        sources = [values[:, at : at + 128] for at in range(0, values.shape[1], 128)]
        taken = []
        for at in range(0, index.shape[1], 128):
            spots = jnp.broadcast_to(index[:, at : at + 128], (rhs, 128))
            low = jnp.bitwise_and(spots, 127)
            high = jnp.right_shift(spots, 7)
            out = jnp.zeros((rhs, 128), F32)
            for k, source in enumerate(sources):
                picked = jnp.take_along_axis(source, low, axis=1, mode="promise_in_bounds")
                out = jnp.where(high == k, picked, out)
            taken.append(out)
        return jnp.concatenate(taken, axis=1)

    def scattered(stage, j, base):
        for group in arriving:
            for entry in group.faces:
                guarded(entry[3], lambda: face_copy(stage, j, group, entry, True).wait_recv())
                block = recv_buf[stage, j, entry[0], height_of(stage)].astype(F32)
                base = base + take(joined(stage, block), inverse_ref[entry[0]])
        return base

    def found(column, targets):
        order = lax.broadcasted_iota(jnp.int32, targets.shape, 0).astype(F32) + 1.0
        matched = jnp.where(column == targets, order, 0.0)
        return jnp.sum(matched, axis=0, keepdims=True).astype(jnp.int32) - 1

    def invert():
        for group in groups:
            for entry in group.faces:
                guarded(entry[3], lambda: map_wait(group, entry).wait_recv())
                cols_ref[pl.ds(entry[0], 1), :] = near_maps[entry[0]]
        turned = jnp.transpose(cols_ref[...].astype(F32))
        targets = lax.broadcasted_iota(jnp.int32, (face, own), 1).astype(F32)
        for group in groups:
            for slot, _, _, _, _ in group.faces:
                inverse_ref[slot] = found(turned[:, slot : slot + 1], targets)

    def send(stage, j, group, values):
        for at, entry in enumerate(group.faces):
            send_buf[stage, j, entry[0], height_of(stage)] = (
                values[:, at * face : (at + 1) * face]
            )

        def start(entry, when=None):
            exists = entry[3]
            if when is not None:
                exists = when if exists is None else jnp.logical_and(exists, when)
            guarded(exists, lambda: face_copy(stage, j, group, entry).start())

        if group is final and len(group.faces) == 2:
            odd = lax.rem(here[group.axis], 2) == 1
            start(group.faces[1], odd)
            start(group.faces[0])
            start(group.faces[1], jnp.logical_not(odd))
        else:
            for entry in group.faces:
                start(entry)

    def precondition(j, ready):
        pair = split(t_ref[...])
        first = True
        for group in sending:
            values = merge(mm(pair, b_ref[:, group.columns]))
            if first:
                ready()
                first = False
            send(0, j, group, rounded(0, values))
        base_ref[...] = merge(mm(pair, b_ref[:, own_columns]))

    def iteration(j, carry):
        start_sums(j)

        pl.when(j == 0)(invert)

        prepared = scattered(0, j, base_ref[...])
        pair = split(prepared)
        for group in sending:
            taken = [take(prepared, near_maps[entry[0]]) for entry in group.faces]
            values = taken[0] if len(taken) == 1 else jnp.concatenate(taken, axis=1)
            send(1, j, group, rounded(1, values))
        pass_sums(j)

        @pl.when(j == 0)
        def _():
            load_own.wait()

        urgent = [group.columns for group in sending if group.axis != 1]
        patient = [group.columns for group in sending if group.axis == 1] + [own_columns]
        for columns in urgent + patient:
            acc_ref[:, columns] = merge(mm(pair, k_ref[own_columns, columns]))

        @pl.when(j == 0)
        def _():
            load_ghosts.wait()

        late = []
        for group in arriving[:-1]:
            values = arrived(1, j, group)
            if group.axis != 1:
                late.append((group, values))
            for columns in urgent + (patient if group.axis == 1 else []):
                acc_ref[:, columns] += joined(1, mm(values, k_ref[group.columns, columns]))
        values = arrived(1, j, final)

        def products(columns):
            rest = [(final, values)]
            if not any(columns is other for other in urgent):
                rest = late + rest
            total = acc_ref[:, columns]
            for group, block in rest:
                total = total + joined(1, mm(block, k_ref[group.columns, columns]))
            return total

        for group in sending:
            send(2, j, group, rounded(2, products(group.columns)))
        base = products(own_columns)
        finish_sums(j)
        coeffs, height = heights(j, ITERS - 1)
        inverse = 1.0 / height
        newest = t_ref[...]
        for k in range(ITERS - 1):
            prepared = prepared - coeffs[k] * z_ref[k]
            newest = newest - coeffs[k] * v_ref[k]
        z_ref[j] = prepared * inverse
        newest = newest * inverse
        v_ref[j] = newest
        last_ref[...] = newest
        applied = scattered(2, j, base)
        for k in range(ITERS - 1):
            applied = applied - coeffs[k] * w_ref[k]
        applied = applied * inverse
        w_ref[j] = applied
        t_ref[...] = applied

        @pl.when(j < ITERS - 1)
        def _():
            precondition(j + 1, lambda: None)

        return carry

    def ready():
        load_own.start()
        load_ghosts.start()

    load_maps.wait()
    pl.semaphore_wait(barrier, expected)
    for group in groups:
        for entry in group.faces:
            guarded(entry[3], lambda: map_copy(group, entry).start())

    load_g.wait()
    t_ref[...] = g_ref[...]
    load_b.wait()
    precondition(0, ready)
    lax.fori_loop(0, ITERS, iteration, 0)
    if direct:
        all_buf[rank(here)] = packed_sums()
        for peer in others:
            all_copy(peer, rank(here)).start()
    else:
        start_sums(ITERS)
        pass_sums(ITERS)
    beta_norm = heights(0, 0)[1]
    rhs_vec = [beta_norm] + [jnp.zeros_like(beta_norm)] * ITERS
    cosines, sines, triangle = [], [], []
    for section in range(ITERS - 1):
        coeffs, height = heights(section + 1, section + 1)
        rotate_column(coeffs + [height], section, cosines, sines, rhs_vec, triangle)
    for group in groups:
        for entry in group.faces:
            def drain():
                map_copy(group, entry).wait_send()
                for stage in range(3):
                    for j in range(ITERS):
                        face_copy(stage, j, group, entry).wait_send()
            guarded(entry[3], drain)
    for r in range(ITERS if direct else ITERS + 1):
        for peer in plane:
            plane_copy(r, peer, ix * ny + iy).wait_send()
        for peer in line:
            line_copy(r, peer, iz).wait_send()
    if direct:
        for peer in others:
            all_copy(peer, rank(here)).wait_send()
        for peer in others:
            all_copy(peer, rank(peer)).wait_recv()
        total = jnp.sum(all_buf[...], axis=0)
        total_ref[ITERS] = jnp.where(mine, total, 0.0)
    else:
        finish_sums(ITERS)
    coeffs, height = heights(ITERS, ITERS)
    rotate_column(coeffs + [height], ITERS - 1, cosines, sines, rhs_vec, triangle)
    solved = back_substitute(rhs_vec, triangle)
    adjoint = solved[0] * z_ref[0]
    for k in range(1, ITERS):
        adjoint = adjoint + solved[k] * z_ref[k]
    out_ref[pl.ds(0, rhs), :] = adjoint
    ratio = jnp.abs(rhs_vec[ITERS]) / beta_norm
    ratio = jnp.sum(jnp.where(rows == lanes, ratio, 0.0), axis=0, keepdims=True)
    out_ref[pl.ds(rhs, 8), pl.ds(0, 128)] = jnp.broadcast_to(ratio, (8, 128))


def local(sizes, gradient, local_schur, inverse_rows, face_maps):
    nx, ny, nz = sizes
    target = gradient[0, 0, 0]
    rhs, own = target.shape
    maps = jnp.swapaxes(face_maps[0, 0], 0, 1)
    face = maps.shape[-1]
    whole = local_schur.shape[-1]
    sums = ITERS + 1
    count = nx * ny * nz
    direct = count if count <= DIRECT_MAX else 1
    vmem = pl.BlockSpec(memory_space=pltpu.VMEM)
    hbm = pl.BlockSpec(memory_space=pl.ANY)
    dma = pltpu.SemaphoreType.DMA
    packed = pl.pallas_call(
        functools.partial(kernel, sizes),
        out_shape=pltpu.VMEM((rhs + 8, own), F32),
        in_specs=[hbm, hbm, hbm, hbm],
        out_specs=vmem,
        scratch_shapes=[
            pltpu.VMEM((rhs, own), F32),
            pltpu.VMEM(maps.shape, jnp.int32),
            pltpu.VMEM((whole, whole), BF16),
            pltpu.VMEM((own, whole), BF16),
            pltpu.VMEM(maps.shape, jnp.int32),
            pltpu.VMEM((8, face), jnp.int32),
            pltpu.VMEM((6, 1, own), jnp.int32),
            pltpu.VMEM((3, ITERS, 6, 2 * rhs, face), BF16),
            pltpu.VMEM((3, ITERS, 6, 2 * rhs, face), BF16),
            pltpu.VMEM((rhs, whole), F32),
            pltpu.VMEM((rhs, own), F32),
            pltpu.VMEM((rhs, own), F32),
            pltpu.VMEM((ITERS, rhs, own), F32),
            pltpu.VMEM((ITERS, rhs, own), F32),
            pltpu.VMEM((ITERS, rhs, own), F32),
            pltpu.VMEM((rhs, own), F32),
            pltpu.VMEM((sums, rhs, 128), F32),
            pltpu.VMEM((sums, nx * ny, 1, 128), F32),
            pltpu.VMEM((sums, nz, 1, 128), F32),
            pltpu.VMEM((direct, 1, 128), F32),
            dma((5,)),
            dma((6,)),
            dma((6,)),
            dma((3, ITERS, 6)),
            dma((3, ITERS, 6)),
            dma((sums, nx * ny)),
            dma((sums, nx * ny)),
            dma((sums, nz)),
            dma((sums, nz)),
            dma((direct,)),
            dma((direct,)),
        ],
        compiler_params=pltpu.CompilerParams(
            collective_id=0, has_side_effects=True, vmem_limit_bytes=56 * 1024 * 1024
        ),
    )(target, maps, local_schur[0, 0, 0], inverse_rows[0, 0, 0])
    return (packed[None, None, None, :rhs], packed[rhs, :rhs])


def solution(mesh):
    placed = P("gx", "gy", "gz", None, None)
    sizes = (mesh.shape["gx"], mesh.shape["gy"], mesh.shape["gz"])
    return jax.shard_map(
        functools.partial(local, sizes),
        mesh=mesh,
        in_specs=(placed, placed, placed, placed),
        out_specs=(placed, P()),
        check_vma=False,
    )
```

```python
import functools

import jax
import jax.numpy as jnp
from jax import lax
from jax.experimental import pallas as pl
from jax.experimental.pallas import tpu as pltpu
from jax.sharding import PartitionSpec as P

ITERS = 3
EPSILON = 1e-06
MESH = pl.DeviceIdType.MESH
BF16 = jnp.bfloat16
F32 = jnp.float32
DIRECT_MAX = 32
PAIRED = (False, True, False)


def split(x):
    high = x.astype(BF16)
    low = (x - high.astype(F32)).astype(BF16)
    return jnp.concatenate([high, low], axis=0)


def merge(x):
    rows = x.shape[0] // 2
    return x[:rows] + x[rows:]


def mm(a, b):
    return jnp.dot(a, b, preferred_element_type=F32)


def rotate_column(column, section, cosines, sines, rhs_vec, triangle):
    column = list(column)
    for earlier in range(section):
        rotated_a = cosines[earlier] * column[earlier] + sines[earlier] * column[earlier + 1]
        rotated_b = -sines[earlier] * column[earlier] + cosines[earlier] * column[earlier + 1]
        column[earlier] = rotated_a
        column[earlier + 1] = rotated_b
    radius = jnp.sqrt(
        column[section] * column[section] + column[section + 1] * column[section + 1]
    )
    cosine = column[section] / radius
    sine_val = column[section + 1] / radius
    column[section] = radius
    cosines.append(cosine)
    sines.append(sine_val)
    rhs_vec[section + 1] = -sine_val * rhs_vec[section]
    rhs_vec[section] = cosine * rhs_vec[section]
    triangle.append(column[: section + 1])


def back_substitute(rhs_vec, triangle):
    num_cols = len(triangle)
    coeffs = [None] * num_cols
    for section in reversed(range(num_cols)):
        running = rhs_vec[section]
        for onward in range(section + 1, num_cols):
            running = running - triangle[onward][section] * coeffs[onward]
        coeffs[section] = running / triangle[section][section]
    return coeffs


class Axis:
    def __init__(self, axis, spot, size, own, face, at):
        self.axis = axis
        self.single = size == 2
        low, high = spot > 0, spot < size - 1
        if self.single:
            which = 2 * axis + jnp.where(low, 0, 1)
            self.faces = [(2 * axis, 2 * axis, which, None, jnp.where(low, -1, 1))]
            self.width = face
            self.start = pl.multiple_of(own + which * face, face)
        else:
            self.faces = [
                (2 * axis, 2 * axis + 1, 2 * axis, low, -1),
                (2 * axis + 1, 2 * axis, 2 * axis + 1, high, 1),
            ]
            self.width = 2 * face
            self.start = own + 2 * axis * face
        self.columns = pl.ds(self.start, self.width)
        self.packed = pl.ds(at, self.width)


def kernel(
    sizes, g_hbm, maps_hbm, k_hbm, b_hbm, out_ref,
    g_ref, maps_ref, k_ref, b_ref, near_maps, cols_ref, inverse_ref, send_buf, recv_buf, acc_ref,
    base_ref, t_ref, v_ref, z_ref, w_ref, last_ref, total_ref, plane_buf, line_buf, all_buf,
    weight_sem, map_send, map_recv, send_sem, recv_sem,
    plane_send, plane_recv, line_send, line_recv, all_send, all_recv,
):
    nx, ny, nz = sizes
    count = nx * ny * nz
    direct = count <= DIRECT_MAX
    rhs, own = g_ref.shape
    face = maps_ref.shape[-1]
    whole = k_ref.shape[0]
    ix, iy, iz = lax.axis_index("gx"), lax.axis_index("gy"), lax.axis_index("gz")
    here = (ix, iy, iz)

    groups = []
    at = 0
    for axis in range(3):
        if sizes[axis] > 1:
            groups.append(Axis(axis, here[axis], sizes[axis], own, face, at))
            at += groups[-1].width
    sending = [group for axis in (0, 2, 1) for group in groups if group.axis == axis]
    arriving = [group for axis in (1, 2, 0) for group in groups if group.axis == axis]
    final = arriving[-1]
    own_columns = pl.ds(0, own)

    def across(axis, step):
        place = list(here)
        place[axis] = place[axis] + step
        return tuple(place)

    def guarded(exists, body):
        if exists is None:
            body()
        else:
            pl.when(exists)(body)

    plane = [
        (lax.rem(ix + dx, nx), lax.rem(iy + dy, ny))
        for dx in range(nx) for dy in range(ny) if dx or dy
    ]
    line = [lax.rem(iz + dz, nz) for dz in range(1, nz)]
    others = [
        (lax.rem(ix + dx, nx), lax.rem(iy + dy, ny), lax.rem(iz + dz, nz))
        for dx in range(nx) for dy in range(ny) for dz in range(nz) if dx or dy or dz
    ]

    load_b = pltpu.make_async_copy(b_hbm, b_ref, weight_sem.at[0])
    load_own = pltpu.make_async_copy(
        k_hbm.at[pl.ds(0, own)], k_ref.at[pl.ds(0, own)], weight_sem.at[1]
    )
    ghosts = pl.ds(own, whole - own)
    load_ghosts = pltpu.make_async_copy(k_hbm.at[ghosts], k_ref.at[ghosts], weight_sem.at[2])
    load_g = pltpu.make_async_copy(g_hbm, g_ref, weight_sem.at[3])
    load_maps = pltpu.make_async_copy(maps_hbm, maps_ref, weight_sem.at[4])
    load_maps.start()
    load_g.start()
    load_b.start()

    barrier = pltpu.get_barrier_semaphore()
    greeted = [((px, py, iz), None) for px, py in plane]
    if nz <= 4:
        greeted += [
            (across(2, dz), iz + dz >= 0 if dz < 0 else iz + dz < nz)
            for dz in (-2, -1, 1, 2) if abs(dz) < nz
        ]
    else:
        greeted += [((ix, iy, pz), None) for pz in line]
    expected = 0
    for peer, exists in greeted:
        expected = expected + (1 if exists is None else exists.astype(jnp.int32))
        guarded(exists, lambda: pl.semaphore_signal(
            barrier, inc=1, device_id=peer, device_id_type=MESH
        ))

    cols_ref[...] = jnp.full(cols_ref.shape, -1, jnp.int32)
    v_ref[...] = jnp.zeros_like(v_ref)
    z_ref[...] = jnp.zeros_like(z_ref)
    w_ref[...] = jnp.zeros_like(w_ref)
    last_ref[...] = jnp.zeros_like(last_ref)
    total_ref[...] = jnp.zeros_like(total_ref)
    for group in groups:
        for slot, _, _, exists, _ in group.faces:
            if exists is not None:
                @pl.when(jnp.logical_not(exists))
                def _():
                    near_maps[slot] = jnp.full(near_maps.shape[1:], -1, jnp.int32)
                    for stage in range(3):
                        for j in range(ITERS):
                            recv_buf[stage, j, slot] = jnp.zeros(recv_buf.shape[3:], BF16)

    def map_copy(group, entry):
        slot, target, which, _, step = entry
        return pltpu.make_async_remote_copy(
            src_ref=maps_ref.at[which], dst_ref=near_maps.at[target],
            send_sem=map_send.at[slot], recv_sem=map_recv.at[target],
            device_id=across(group.axis, step), device_id_type=MESH,
        )

    def map_wait(group, entry):
        slot, _, which, _, step = entry
        return pltpu.make_async_remote_copy(
            src_ref=maps_ref.at[which], dst_ref=near_maps.at[slot],
            send_sem=map_send.at[slot], recv_sem=map_recv.at[slot],
            device_id=across(group.axis, step), device_id_type=MESH,
        )

    def height_of(stage):
        return pl.ds(0, 2 * rhs if PAIRED[stage] else rhs)

    def face_copy(stage, j, group, entry, arrival=False):
        slot, target, _, _, step = entry
        into = slot if arrival else target
        return pltpu.make_async_remote_copy(
            src_ref=send_buf.at[stage, j, slot, height_of(stage)],
            dst_ref=recv_buf.at[stage, j, into, height_of(stage)],
            send_sem=send_sem.at[stage, j, slot], recv_sem=recv_sem.at[stage, j, into],
            device_id=across(group.axis, step), device_id_type=MESH,
        )

    def plane_copy(r, peer, slot):
        mine = ix * ny + iy
        return pltpu.make_async_remote_copy(
            src_ref=plane_buf.at[r, mine], dst_ref=plane_buf.at[r, slot],
            send_sem=plane_send.at[r, peer[0] * ny + peer[1]], recv_sem=plane_recv.at[r, slot],
            device_id=(peer[0], peer[1], iz), device_id_type=MESH,
        )

    def line_copy(r, peer, slot):
        return pltpu.make_async_remote_copy(
            src_ref=line_buf.at[r, iz], dst_ref=line_buf.at[r, slot],
            send_sem=line_send.at[r, peer], recv_sem=line_recv.at[r, slot],
            device_id=(ix, iy, peer), device_id_type=MESH,
        )

    def rank(peer):
        return (peer[0] * ny + peer[1]) * nz + peer[2]

    def all_copy(peer, slot):
        return pltpu.make_async_remote_copy(
            src_ref=all_buf.at[rank(here)], dst_ref=all_buf.at[slot],
            send_sem=all_send.at[rank(peer)], recv_sem=all_recv.at[slot],
            device_id=peer, device_id_type=MESH,
        )

    lanes = lax.broadcasted_iota(jnp.int32, (rhs, 128), 1)
    rows = lax.broadcasted_iota(jnp.int32, (rhs, 128), 0)
    spread = 128 // rhs
    places = lax.rem(lanes, spread)
    mine = lax.div(lanes, spread) == rows

    def packed_sums():
        t = t_ref[...]
        last = last_ref[...]
        packed = jnp.where(places == ITERS, jnp.sum(t * t, axis=1, keepdims=True), 0.0)
        for k in range(ITERS):
            v = v_ref[k]
            packed = jnp.where(places == k, jnp.sum(v * t, axis=1, keepdims=True), packed)
            packed = jnp.where(
                places == ITERS + 1 + k, jnp.sum(v * last, axis=1, keepdims=True), packed
            )
        return jnp.sum(jnp.where(mine, packed, 0.0), axis=0, keepdims=True)

    def start_sums(r):
        plane_buf[r, ix * ny + iy] = packed_sums()
        for peer in plane:
            plane_copy(r, peer, ix * ny + iy).start()

    def pass_sums(r):
        for peer in plane:
            plane_copy(r, peer, peer[0] * ny + peer[1]).wait_recv()
        partial = plane_buf[r, 0]
        for at in range(1, nx * ny):
            partial = partial + plane_buf[r, at]
        line_buf[r, iz] = partial
        for peer in line:
            line_copy(r, peer, iz).start()

    def finish_sums(r):
        for peer in line:
            line_copy(r, peer, peer).wait_recv()
        total = line_buf[r, 0]
        for at in range(1, nz):
            total = total + line_buf[r, at]
        total_ref[r] = jnp.where(mine, total, 0.0)

    def pick(r, lane):
        return jnp.sum(jnp.where(places == lane, total_ref[r], 0.0), axis=1, keepdims=True)

    def heights(r, count):
        coeffs = [pick(r, k) for k in range(count)]
        running = pick(r, ITERS)
        for k in range(count):
            running = running - 2.0 * coeffs[k] * coeffs[k]
            for n in range(k + 1):
                element = coeffs[k] * pick(k + 1, ITERS + 1 + n) * coeffs[n]
                running = running + (element if n == k else 2.0 * element)
        return coeffs, jnp.sqrt(jnp.maximum(running, 0.0) + EPSILON)

    def arrived(stage, j, group):
        for entry in group.faces:
            guarded(entry[3], lambda: face_copy(stage, j, group, entry, True).wait_recv())
        blocks = [recv_buf[stage, j, entry[0], height_of(stage)] for entry in group.faces]
        return blocks[0] if len(blocks) == 1 else jnp.concatenate(blocks, axis=1)

    def joined(stage, product):
        return merge(product) if PAIRED[stage] else product

    def rounded(stage, values):
        return split(values) if PAIRED[stage] else values.astype(BF16)

    def take(values, index):
        sources = [values[:, at : at + 128] for at in range(0, values.shape[1], 128)]
        taken = []
        for at in range(0, index.shape[1], 128):
            spots = jnp.broadcast_to(index[:, at : at + 128], (rhs, 128))
            low = jnp.bitwise_and(spots, 127)
            high = jnp.right_shift(spots, 7)
            out = jnp.zeros((rhs, 128), F32)
            for k, source in enumerate(sources):
                picked = jnp.take_along_axis(source, low, axis=1, mode="promise_in_bounds")
                out = jnp.where(high == k, picked, out)
            taken.append(out)
        return jnp.concatenate(taken, axis=1)

    def scattered(stage, j, base):
        for group in arriving:
            for entry in group.faces:
                guarded(entry[3], lambda: face_copy(stage, j, group, entry, True).wait_recv())
                block = recv_buf[stage, j, entry[0], height_of(stage)].astype(F32)
                base = base + take(joined(stage, block), inverse_ref[entry[0]])
        return base

    def found(column, targets):
        order = lax.broadcasted_iota(jnp.int32, targets.shape, 0).astype(F32) + 1.0
        matched = jnp.where(column == targets, order, 0.0)
        return jnp.sum(matched, axis=0, keepdims=True).astype(jnp.int32) - 1

    def invert():
        for group in groups:
            for entry in group.faces:
                guarded(entry[3], lambda: map_wait(group, entry).wait_recv())
                cols_ref[pl.ds(entry[0], 1), :] = near_maps[entry[0]]
        turned = jnp.transpose(cols_ref[...].astype(F32))
        targets = lax.broadcasted_iota(jnp.int32, (face, own), 1).astype(F32)
        for group in groups:
            for slot, _, _, _, _ in group.faces:
                inverse_ref[slot] = found(turned[:, slot : slot + 1], targets)

    def send(stage, j, group, values):
        for at, entry in enumerate(group.faces):
            send_buf[stage, j, entry[0], height_of(stage)] = (
                values[:, at * face : (at + 1) * face]
            )

        def start(entry, when=None):
            exists = entry[3]
            if when is not None:
                exists = when if exists is None else jnp.logical_and(exists, when)
            guarded(exists, lambda: face_copy(stage, j, group, entry).start())

        if group is final and len(group.faces) == 2:
            odd = lax.rem(here[group.axis], 2) == 1
            start(group.faces[1], odd)
            start(group.faces[0])
            start(group.faces[1], jnp.logical_not(odd))
        else:
            for entry in group.faces:
                start(entry)

    def precondition(j, ready):
        pair = split(t_ref[...])
        first = True
        for group in sending:
            values = merge(mm(pair, b_ref[:, group.columns]))
            if first:
                ready()
                first = False
            send(0, j, group, rounded(0, values))
        base_ref[...] = merge(mm(pair, b_ref[:, own_columns]))

    def iteration(j, carry):
        start_sums(j)

        pl.when(j == 0)(invert)

        prepared = scattered(0, j, base_ref[...])
        pair = split(prepared)
        for group in sending:
            taken = [take(prepared, near_maps[entry[0]]) for entry in group.faces]
            values = taken[0] if len(taken) == 1 else jnp.concatenate(taken, axis=1)
            send(1, j, group, rounded(1, values))

        @pl.when(j == 0)
        def _():
            load_own.wait()

        urgent = [group.columns for group in sending if group.axis != 1]
        patient = [group.columns for group in sending if group.axis == 1] + [own_columns]
        for columns in urgent + patient:
            acc_ref[:, columns] = merge(mm(pair, k_ref[own_columns, columns]))
        pass_sums(j)

        @pl.when(j == 0)
        def _():
            load_ghosts.wait()

        late = []
        for group in arriving[:-1]:
            values = arrived(1, j, group)
            if group.axis != 1:
                late.append((group, values))
            for columns in urgent + (patient if group.axis == 1 else []):
                acc_ref[:, columns] += joined(1, mm(values, k_ref[group.columns, columns]))
        values = arrived(1, j, final)

        def products(columns):
            rest = [(final, values)]
            if not any(columns is other for other in urgent):
                rest = late + rest
            total = acc_ref[:, columns]
            for group, block in rest:
                total = total + joined(1, mm(block, k_ref[group.columns, columns]))
            return total

        for group in sending:
            send(2, j, group, rounded(2, products(group.columns)))
        base = products(own_columns)
        finish_sums(j)
        coeffs, height = heights(j, ITERS - 1)
        inverse = 1.0 / height
        newest = t_ref[...]
        for k in range(ITERS - 1):
            prepared = prepared - coeffs[k] * z_ref[k]
            newest = newest - coeffs[k] * v_ref[k]
        z_ref[j] = prepared * inverse
        newest = newest * inverse
        v_ref[j] = newest
        last_ref[...] = newest
        applied = scattered(2, j, base)
        for k in range(ITERS - 1):
            applied = applied - coeffs[k] * w_ref[k]
        applied = applied * inverse
        w_ref[j] = applied
        t_ref[...] = applied

        @pl.when(j < ITERS - 1)
        def _():
            precondition(j + 1, lambda: None)

        return carry

    def ready():
        load_own.start()
        load_ghosts.start()

    load_maps.wait()
    pl.semaphore_wait(barrier, expected)
    for group in groups:
        for entry in group.faces:
            guarded(entry[3], lambda: map_copy(group, entry).start())

    load_g.wait()
    t_ref[...] = g_ref[...]
    load_b.wait()
    precondition(0, ready)
    lax.fori_loop(0, ITERS, iteration, 0)
    if direct:
        all_buf[rank(here)] = packed_sums()
        for peer in others:
            all_copy(peer, rank(here)).start()
    else:
        start_sums(ITERS)
        pass_sums(ITERS)
    beta_norm = heights(0, 0)[1]
    rhs_vec = [beta_norm] + [jnp.zeros_like(beta_norm)] * ITERS
    cosines, sines, triangle = [], [], []
    for section in range(ITERS - 1):
        coeffs, height = heights(section + 1, section + 1)
        rotate_column(coeffs + [height], section, cosines, sines, rhs_vec, triangle)
    for group in groups:
        for entry in group.faces:
            def drain():
                map_copy(group, entry).wait_send()
                for stage in range(3):
                    for j in range(ITERS):
                        face_copy(stage, j, group, entry).wait_send()
            guarded(entry[3], drain)
    for r in range(ITERS if direct else ITERS + 1):
        for peer in plane:
            plane_copy(r, peer, ix * ny + iy).wait_send()
        for peer in line:
            line_copy(r, peer, iz).wait_send()
    if direct:
        for peer in others:
            all_copy(peer, rank(here)).wait_send()
        for peer in others:
            all_copy(peer, rank(peer)).wait_recv()
        total = jnp.sum(all_buf[...], axis=0)
        total_ref[ITERS] = jnp.where(mine, total, 0.0)
    else:
        finish_sums(ITERS)
    coeffs, height = heights(ITERS, ITERS)
    rotate_column(coeffs + [height], ITERS - 1, cosines, sines, rhs_vec, triangle)
    solved = back_substitute(rhs_vec, triangle)
    adjoint = solved[0] * z_ref[0]
    for k in range(1, ITERS):
        adjoint = adjoint + solved[k] * z_ref[k]
    out_ref[pl.ds(0, rhs), :] = adjoint
    ratio = jnp.abs(rhs_vec[ITERS]) / beta_norm
    ratio = jnp.sum(jnp.where(rows == lanes, ratio, 0.0), axis=0, keepdims=True)
    out_ref[pl.ds(rhs, 8), pl.ds(0, 128)] = jnp.broadcast_to(ratio, (8, 128))


def local(sizes, gradient, local_schur, inverse_rows, face_maps):
    nx, ny, nz = sizes
    target = gradient[0, 0, 0]
    rhs, own = target.shape
    maps = jnp.swapaxes(face_maps[0, 0], 0, 1)
    face = maps.shape[-1]
    whole = local_schur.shape[-1]
    sums = ITERS + 1
    count = nx * ny * nz
    direct = count if count <= DIRECT_MAX else 1
    vmem = pl.BlockSpec(memory_space=pltpu.VMEM)
    hbm = pl.BlockSpec(memory_space=pl.ANY)
    dma = pltpu.SemaphoreType.DMA
    packed = pl.pallas_call(
        functools.partial(kernel, sizes),
        out_shape=pltpu.VMEM((rhs + 8, own), F32),
        in_specs=[hbm, hbm, hbm, hbm],
        out_specs=vmem,
        scratch_shapes=[
            pltpu.VMEM((rhs, own), F32),
            pltpu.VMEM(maps.shape, jnp.int32),
            pltpu.VMEM((whole, whole), BF16),
            pltpu.VMEM((own, whole), BF16),
            pltpu.VMEM(maps.shape, jnp.int32),
            pltpu.VMEM((8, face), jnp.int32),
            pltpu.VMEM((6, 1, own), jnp.int32),
            pltpu.VMEM((3, ITERS, 6, 2 * rhs, face), BF16),
            pltpu.VMEM((3, ITERS, 6, 2 * rhs, face), BF16),
            pltpu.VMEM((rhs, whole), F32),
            pltpu.VMEM((rhs, own), F32),
            pltpu.VMEM((rhs, own), F32),
            pltpu.VMEM((ITERS, rhs, own), F32),
            pltpu.VMEM((ITERS, rhs, own), F32),
            pltpu.VMEM((ITERS, rhs, own), F32),
            pltpu.VMEM((rhs, own), F32),
            pltpu.VMEM((sums, rhs, 128), F32),
            pltpu.VMEM((sums, nx * ny, 1, 128), F32),
            pltpu.VMEM((sums, nz, 1, 128), F32),
            pltpu.VMEM((direct, 1, 128), F32),
            dma((5,)),
            dma((6,)),
            dma((6,)),
            dma((3, ITERS, 6)),
            dma((3, ITERS, 6)),
            dma((sums, nx * ny)),
            dma((sums, nx * ny)),
            dma((sums, nz)),
            dma((sums, nz)),
            dma((direct,)),
            dma((direct,)),
        ],
        compiler_params=pltpu.CompilerParams(
            collective_id=0, has_side_effects=True, vmem_limit_bytes=56 * 1024 * 1024
        ),
    )(target, maps, local_schur[0, 0, 0], inverse_rows[0, 0, 0])
    return (packed[None, None, None, :rhs], packed[rhs, :rhs])


def solution(mesh):
    placed = P("gx", "gy", "gz", None, None)
    sizes = (mesh.shape["gx"], mesh.shape["gy"], mesh.shape["gz"])
    return jax.shard_map(
        functools.partial(local, sizes),
        mesh=mesh,
        in_specs=(placed, placed, placed, placed),
        out_specs=(placed, P()),
        check_vma=False,
    )
```
